256 devices in a mesh: leaf: 64 (over x, z, core), cols: 4 (over y).
Axes of the slice: x: 4, y: 4, z: 8, core: 2. Of those that a mesh axis runs over, the one named last changes fastest.
Arguments:
- samples: bfloat16 [2048, 131072], P('cols', 'leaf'), may hold values from -6 to 6
- order_perm: int32 [131072], P('leaf'), may hold values from 0 to 131071, as said below
- leaf_factor: bfloat16 [128, 1024, 1024], P('leaf'), may hold values from -0.1875 to 0.1875
- bases: bfloat16 [7, 64, 131072], P(None, None, 'leaf'), may hold values from -110 to 110
- coupling: float32 [7, 64, 64, 64], P(None, 'leaf'), may hold values from -1 to 1, as said below
- ranks: int32 [7, 128], replicated, may hold values from 16 to 64
Outputs:
- transformed: float32 [2048, 131072], P('cols', 'leaf')
The draws below stay inside these ranges and needn't reach their ends.
Inputs may be any that keep to these rules, and one draw needn't show every extreme that they name: `order_perm`: each aligned block of 2048 positions holds a permutation of the same block's indices. coupling[l, d] equals coupling[l, e] whenever d and e lie in the same level-l node, that is d // 2**l == e // 2**l.
All inputs are finite; a program needn't handle non-finite values.
Results may differ from the reference program's by a relative error of at most 0.0003.
Values sent between devices are 32-bit elements; how exact they have to be, the bound alone decides.
No kernel may reach another device: no remote copies, remote signals or barrier semaphores. Data moves between devices by JAX's collectives and lax.ppermute only.
A program may use at most 128 MiB of HBM per device.

```python
import jax
import jax.numpy as jnp
from jax import lax

LEAF = 1024
R = 64
ROWS_DEV = 2048
ORDER = 131072
NLEAVES = 128
NCOLS = 2048
LEVELS = 7


def draw_order_perm(key, part):
    devices = ORDER // ROWS_DEV
    keys = jax.random.split(jax.random.fold_in(key, 11), devices)
    perms = jax.vmap(lambda one_key: jax.random.permutation(one_key, ROWS_DEV))(keys)
    offsets = jnp.arange(devices, dtype=jnp.int32)[:, None] * ROWS_DEV
    return (perms.astype(jnp.int32) + offsets).reshape(-1).astype(jnp.int32)


def draw_coupling(key, part):
    devices = ORDER // ROWS_DEV
    inner_key = jax.random.fold_in(key, 23)
    base = jax.random.normal(inner_key, (LEVELS, devices, R, R), jnp.float32) / R ** 0.5
    base = jnp.clip(base, -1.0, 1.0)
    shifts = jnp.arange(LEVELS, dtype=jnp.int32)[:, None]
    source = jnp.arange(devices, dtype=jnp.int32)[None, :] >> shifts << shifts
    picked = jax.vmap(lambda level_base, level_source: level_base[level_source])(base, source)
    return picked.astype(jnp.float32)


def draw_bases(key, part):
    devices = ORDER // ROWS_DEV
    entry_key = jax.random.fold_in(key, 31)
    factor_key = jax.random.fold_in(key, 37)
    position = jnp.arange(devices, dtype=jnp.float32) / max(devices - 1, 1)
    entries = jnp.clip(jax.random.normal(entry_key, (LEVELS, R, devices, ROWS_DEV), jnp.float32), -6.0, 6.0)
    rising = 3.0 ** position
    factors = jax.random.uniform(factor_key, (LEVELS, 1, devices, 1), jnp.float32, 1.0, 2.0)
    scaled = entries * factors * rising[None, None, :, None]
    return scaled.reshape(LEVELS, R, ORDER).astype(jnp.bfloat16)


def touch_ends(values, rng, smallest, high):
    spot = [jax.random.randint(jax.random.fold_in(rng, axis), (), 0, length) for axis, length in enumerate(values.shape)]
    main_axis = values.shape.index(max(values.shape))
    neighbour = spot[:main_axis] + [(spot[main_axis] + 1) % values.shape[main_axis]] + spot[main_axis + 1:]
    return values.at[tuple(spot)].set(smallest).at[tuple(neighbour)].set(high)


def shard_levels(rng, shape, shards, low, top_value):
    def one(axis_at, shards_of):
        steps = jax.random.uniform(jax.random.fold_in(jax.random.fold_in(rng, 6), axis_at), (shards_of,), jnp.float32, low / len(shards), top_value / len(shards))
        return jnp.repeat(jnp.exp(steps), shape[axis_at] // shards_of).reshape((-1,) + (1,) * (len(shape) - axis_at - 1))

    loudness = one(*shards[0])
    for cut in shards[1:]:
        loudness = loudness * one(*cut)
    return loudness


def normal_values(own_key, extent, scale, most, shards=(), kind=jnp.bfloat16):
    factor_of = shard_levels(own_key, extent, shards, -0.22, 0.18) if shards else 1.0
    drawn = jax.random.normal(own_key, extent, jnp.float32) * scale * factor_of
    return jnp.minimum(jnp.maximum(drawn, -most), most).astype(kind)


def setup_inputs(seed: int = 0) -> dict:
    seeds = jax.random.split(jax.random.key(seed), 7)
    samples = normal_values(seeds[0], (NCOLS, ORDER), 1.0, 6.0, ((0, 4), (1, 64)))
    order_perm = draw_order_perm(jax.random.fold_in(seeds[6], 71), 0)
    leaf_factor = normal_values(seeds[2], (NLEAVES, LEAF, LEAF), LEAF ** -0.5, 0.1875, ((0, 64),))
    bases = draw_bases(jax.random.fold_in(seeds[6], 71), 0)
    coupling = draw_coupling(jax.random.fold_in(seeds[6], 71), 0)
    ranks = touch_ends(jax.random.randint(seeds[5], (LEVELS, NLEAVES), R // 4, R + 1), jax.random.fold_in(seeds[5], 1), R // 4, R).astype(jnp.int32)
    return dict(samples=samples, order_perm=order_perm, leaf_factor=leaf_factor, bases=bases, coupling=coupling, ranks=ranks)


HIGH = lax.Precision.HIGHEST

def chol_apply(system, right_side):
    lower_factor = jnp.linalg.cholesky(system)
    middle = lax.linalg.triangular_solve(lower_factor, right_side, left_side=True, lower=True)
    return lax.linalg.triangular_solve(lower_factor, middle, left_side=True, lower=True, transpose_a=True)

def coupled(coupling_now, gram_other, proj_other):
    rank_width = coupling_now.shape[-1]
    inner = jnp.matmul(coupling_now, gram_other, precision=HIGH)
    system = jnp.eye(rank_width, dtype=jnp.float32) + jnp.matmul(inner, jnp.swapaxes(coupling_now, -1, -2), precision=HIGH)
    return chol_apply(system, jnp.matmul(coupling_now, proj_other, precision=HIGH))

def leaf_product(leaf_pair):
    return jnp.dot(leaf_pair[0].astype(jnp.float32), leaf_pair[1].astype(jnp.float32), preferred_element_type=jnp.float32)

def reference(samples, order_perm, leaf_factor, bases, coupling, ranks):
    permuted = jnp.take(samples, order_perm, axis=1)
    blocks = jnp.swapaxes(permuted.reshape(NCOLS, NLEAVES, LEAF), 0, 1)
    leaf_out = lax.map(leaf_product, (blocks, leaf_factor))
    field = jnp.swapaxes(leaf_out, 0, 1).reshape(NCOLS, ORDER)
    for tree_level in range(LEVELS):
        child_rows = LEAF * 2 ** tree_level
        nodes = ORDER // (2 * child_rows)
        scale = 1.0 / child_rows ** 0.5
        state = field.reshape(NCOLS, nodes, 2, child_rows)
        ranks_here = ranks[tree_level, ::2 ** tree_level].reshape(nodes, 2)
        column_mask = (jnp.arange(R, dtype=jnp.int32)[None, None, :] < ranks_here[:, :, None]).astype(jnp.float32) * scale
        basis = bases[tree_level].astype(jnp.float32).reshape(R, nodes, 2, child_rows)
        basis = basis * jnp.transpose(column_mask, (2, 0, 1))[..., None]
        proj = jnp.einsum('rmkc,jmkc->mkrj', basis, state, precision=HIGH)
        gram = jnp.einsum('rmkc,smkc->mkrs', basis, basis, precision=HIGH)
        links = coupling[tree_level, ::2 ** tree_level]
        first_update = coupled(links, gram[:, 1], proj[:, 1])
        second_update = coupled(jnp.swapaxes(links, -1, -2), gram[:, 0], proj[:, 0])
        updates = jnp.stack([first_update, second_update], axis=1)
        state = state - jnp.einsum('mkrj,rmkc->jmkc', updates, basis, precision=HIGH)
        field = state.reshape(NCOLS, ORDER)
    return field
```

```python
import functools
import math

import jax
import jax.numpy as jnp
from jax import lax
from jax.experimental import pallas as pl
from jax.experimental.pallas import tpu as pltpu
from jax.sharding import PartitionSpec as P

F32, BF16 = jnp.float32, jnp.bfloat16
HIGH = lax.Precision.HIGHEST
NT = (((1,), (1,)), ((), ()))
NN = (((1,), (0,)), ((), ()))
TN = (((0,), (0,)), ((), ()))

LEAF, R, ROWS, COLS, LEVELS = 1024, 64, 2048, 512, 7
UP = (LEVELS - 1) * R
BLK = 256
MIB = 1024 * 1024
VMEM = pl.BlockSpec(memory_space=pltpu.VMEM)
SMEM = pl.BlockSpec(memory_space=pltpu.SMEM)


def params(mib, **more):
    return pltpu.CompilerParams(vmem_limit_bytes=mib * MIB, **more)


def cost(flops, moved):
    return pl.CostEstimate(flops=int(flops), bytes_accessed=int(moved), transcendentals=0)


def shape(*dims, dtype=F32):
    return jax.ShapeDtypeStruct(dims, dtype)


def split(value):
    high = value.astype(BF16)
    return high, (value - high.astype(F32)).astype(BF16)


def dot(left, right, dims):
    return lax.dot_general(left, right, dims, preferred_element_type=F32)


def dot_high(left, right, dims):
    return lax.dot_general(left, right, dims, precision=HIGH, preferred_element_type=F32)


def twice(value, axis):
    return jnp.concatenate([value, value], axis=axis)


def gram_kernel(bases_ref, tiles_ref, first_ref, gram0_ref, cross0_ref):
    upper = bases_ref[1:].reshape(UP, ROWS)
    gram = dot(upper, upper, NT)
    first_ref[...] = gram[:R]
    for part in range(8):
        tile = 0
        for level in range(6):
            top = level * R + 8 * part
            for lane in range(level // 2, 3):
                tiles_ref[part, tile] = gram[top:top + 8, lane * 128:lane * 128 + 128]
                tile += 1
    for half in range(2):
        columns = slice(half * LEAF, (half + 1) * LEAF)
        base0 = bases_ref[0, :, columns]
        gram0_ref[half] = dot(base0, base0, NT)
        cross0_ref[half] = dot(base0, bases_ref[1:, :, columns].reshape(UP, LEAF), NT)


def grams(bases):
    return pl.pallas_call(
        gram_kernel,
        out_shape=(shape(8, 12, 8, 128), shape(R, UP), shape(2, R, R), shape(2, R, UP)),
        in_specs=[VMEM],
        out_specs=(VMEM,) * 4,
        compiler_params=params(12),
        cost_estimate=cost(2 * UP * UP * ROWS * 1.2, 4e6),
        name="gram",
    )(bases)


def permute_kernel(samples_ref, order_ref, out_ref):
    rows = lax.broadcasted_iota(jnp.int32, (ROWS, BLK), 0)
    local = jnp.bitwise_and(order_ref[...], ROWS - 1)
    chosen = (rows == local).astype(F32).astype(BF16)
    out_ref[...] = dot(samples_ref[...], chosen, NN).astype(BF16)


def permute(samples, order):
    return pl.pallas_call(
        permute_kernel,
        grid=(ROWS // BLK,),
        out_shape=shape(COLS, ROWS, dtype=BF16),
        in_specs=[
            pl.BlockSpec((COLS, ROWS), lambda j: (0, 0)),
            pl.BlockSpec((1, BLK), lambda j: (0, j)),
        ],
        out_specs=pl.BlockSpec((COLS, BLK), lambda j: (0, j)),
        compiler_params=params(16),
        cost_estimate=cost(2 * COLS * ROWS * ROWS, 4e6),
        name="permute",
    )(samples, order)


def leaf_kernel(permuted_ref, factor_ref, bases_ref, field_ref, q0_ref, q_ref):
    half, step = pl.program_id(0), pl.program_id(1)

    @pl.when((half == 0) & (step == 0))
    def _():
        q0_ref[...] = jnp.zeros_like(q0_ref)
        q_ref[...] = jnp.zeros_like(q_ref)

    field = dot(permuted_ref[...], factor_ref[0], NN)
    field_ref[...] = field
    high, low = split(field)
    upper = bases_ref[1:].reshape(UP, BLK)
    q_ref[...] += dot(high, upper, NT) + dot(low, upper, NT)
    base0 = bases_ref[0]
    nothing = jnp.zeros_like(base0)
    placed = jnp.concatenate(
        [jnp.where(half == 0, base0, nothing), jnp.where(half == 0, nothing, base0)], axis=0
    )
    q0_ref[...] += dot(high, placed, NT) + dot(low, placed, NT)


def leaf_project(permuted, factor, bases):
    steps = LEAF // BLK
    return pl.pallas_call(
        leaf_kernel,
        grid=(2, steps),
        out_shape=(shape(COLS, ROWS), shape(COLS, 128), shape(COLS, UP)),
        in_specs=[
            pl.BlockSpec((COLS, LEAF), lambda h, j: (0, h)),
            pl.BlockSpec((1, LEAF, BLK), lambda h, j: (h, 0, j)),
            pl.BlockSpec((LEVELS, R, BLK), lambda h, j: (0, 0, h * steps + j)),
        ],
        out_specs=(
            pl.BlockSpec((COLS, BLK), lambda h, j: (0, h * steps + j)),
            pl.BlockSpec((COLS, 128), lambda h, j: (0, 0)),
            pl.BlockSpec((COLS, UP), lambda h, j: (0, 0)),
        ),
        compiler_params=params(20),
        cost_estimate=cost(2 * COLS * ROWS * (LEAF + 900), 12e6),
        name="leaf",
    )(permuted, factor, bases)


def coupling_forms(link):
    flipped = link.T
    plain = twice(flipped, 0).T
    return plain, twice(link, 0).T


def lanes(rows=R):
    return lax.broadcasted_iota(jnp.int32, (rows, 128), 1)


def system(link_dup, gram_tile, upper_half, rank_own, scale):
    lane = lanes()
    joint = jnp.where(jnp.bitwise_and(lane, R - 1) < rank_own, link_dup * scale, 0.0)
    placed = jnp.where((lane >= R) == upper_half, joint, 0.0)
    inner = dot_high(gram_tile, twice(placed, 0), NT)
    outer = dot_high(joint[:, :R], inner, NN)
    row = lax.broadcasted_iota(jnp.int32, (R, 128), 0)
    outer = outer + jnp.where(row == lane, 1.0, 0.0)
    return jnp.where(lane < R, outer, joint)


def eliminate(work_ref, count):
    row = lax.broadcasted_iota(jnp.int32, (R, 128), 0)

    def block(step, carry):
        top = pl.multiple_of(step * 8, 8)
        for item in range(count):
            value = work_ref[item]
            spread = [jnp.broadcast_to(value[:, j:j + 1], (R, 128)) for j in range(8)]
            tile = work_ref[item, pl.ds(top, 8), :]
            tile_row = lax.broadcasted_iota(jnp.int32, (8, 128), 0)
            heads = [jnp.broadcast_to(tile[:, j:j + 1], (8, 128)) for j in range(8)]
            for j in range(8):
                inverse = 1.0 / heads[j][j:j + 1, :]
                pivot = tile[j:j + 1, :] * inverse
                here = row == top + j
                value = jnp.where(here, pivot, value - spread[j] * pivot)
                tile_next = jnp.where(tile_row == j, pivot, tile - heads[j] * pivot)
                for i in range(j + 1, 8):
                    element = heads[i][j:j + 1, :] * inverse
                    spread[i] = jnp.where(here, element, spread[i] - spread[j] * element)
                    heads[i] = jnp.where(tile_row == j, element, heads[i] - heads[j] * element)
                tile = tile_next
            work_ref[item] = pltpu.roll(value, 120, 1)
        return carry

    lax.fori_loop(0, 8, block, 0)


def solved(work_ref, item, rank_sibling, scale):
    row = lax.broadcasted_iota(jnp.int32, (R, 128), 0)
    keep = (row < rank_sibling) & (lanes() < R)
    return jnp.where(keep, work_ref[item] * scale, 0.0)


def pair(value):
    high, low = split(value)
    return jnp.concatenate([high, low], axis=1)


def apply_nt(value_pair, weight):
    high, low = split(weight)
    return dot(value_pair, twice(high, 1), NT) + dot(value_pair, twice(low, 1), NT)


def apply_nn(value_pair, weight):
    high, low = split(weight)
    return dot(value_pair, twice(high, 0), NN) + dot(value_pair, twice(low, 0), NN)


def packed(value_pair, weight, half):
    nothing = jnp.zeros_like(weight)
    start = half * 256
    return apply_nt(value_pair[start:start + 128], jnp.concatenate([weight, nothing], 0)) + apply_nt(
        value_pair[start + 128:start + 256], jnp.concatenate([nothing, weight], 0)
    )


def scale_of(level):
    return 1.0 / math.sqrt(LEAF * 2**level)


def early_kernel(ranks_ref, link_ref, gram0_ref, cross0_ref, own1_ref, sib1_ref, q0_ref, q_ref,
                 u0_ref, u1_ref, x_ref, work_ref):
    leaf = lax.axis_index("leaf")
    second = jnp.bitwise_and(leaf, 1)
    plain0, flipped0 = coupling_forms(link_ref[0, 0])
    plain1, flipped1 = coupling_forms(link_ref[1, 0])
    rank_f, rank_s = ranks_ref[0, 2 * leaf], ranks_ref[0, 2 * leaf + 1]
    rank_1, rank_1s = ranks_ref[1, 2 * leaf], ranks_ref[1, 2 * jnp.bitwise_xor(leaf, 1)]
    scale0, scale1 = scale_of(0), scale_of(1)
    nothing = jnp.zeros((R, R), F32)
    work_ref[0] = system(flipped0, jnp.concatenate([gram0_ref[0], nothing], 1), False, rank_f, scale0)
    work_ref[1] = system(plain0, jnp.concatenate([gram0_ref[1], nothing], 1), False, rank_s, scale0)
    work_ref[2] = system(jnp.where(second == 1, plain1, flipped1), own1_ref[:, :128], False, rank_1, scale1)
    eliminate(work_ref, 3)
    from_first = solved(work_ref, 0, rank_s, scale0)
    from_second = pltpu.roll(solved(work_ref, 1, rank_f, scale0), R, 1)
    u0 = apply_nt(pair(q0_ref[...]), jnp.concatenate([from_second, from_first], 0))
    u0_ref[...] = u0
    x_ref[...] = q_ref[...] - apply_nn(pair(u0), cross0_ref[...].reshape(128, UP))
    weight = solved(work_ref, 2, rank_1s, scale1)
    value = pair(x_ref[:, :128])
    u1_ref[0] = packed(value, weight, 0)
    u1_ref[1] = packed(value, weight, 1)
    onward = dot_high(weight, sib1_ref[...], TN)
    x_ref[...] -= apply_nn(value, onward)


def early(ranks, coupling, gram0, cross0, own1, sib1, q0, q):
    return pl.pallas_call(
        early_kernel,
        out_shape=(shape(COLS, 128), shape(2, 128, 128), shape(COLS, UP)),
        in_specs=[SMEM] + [VMEM] * 7,
        out_specs=(VMEM,) * 3,
        scratch_shapes=[pltpu.VMEM((3, R, 128), F32)],
        compiler_params=params(20),
        cost_estimate=cost(3e9, 4e6),
        name="early",
    )(ranks, coupling, gram0, cross0, own1, sib1, q0, q)


OWN_TILE = {2: 0, 3: 3, 4: 5, 5: 7, 6: 8}
ONWARD = {2: ((1, 1), (2, 2)), 3: ((3, 1), (4, 2)), 4: ((6, 2),), 5: ((7, 2),), 6: ()}


def late_kernel(ranks_ref, link_ref, near_ref, far_ref, x_in_ref, keep_ref, send_ref, pk_ref, x_ref, work_ref):
    leaf, col = lax.axis_index("leaf"), lax.axis_index("cols")
    core = jnp.bitwise_and(leaf, 1)
    for other, source in ((0, near_ref), (1, far_ref)):
        for offset in range(4):
            part = jnp.bitwise_xor(core, other) * 4 + jnp.bitwise_xor(col, offset)
            rows = pl.ds(pl.multiple_of(part * 8, 8), 8)
            for tile in range(9):
                pk_ref[tile, rows, :] = source[offset, tile]
    for level in range(2, 7):
        child = jnp.right_shift(leaf, level - 1)
        plain, flipped = coupling_forms(link_ref[level, 0])
        rank = ranks_ref[level, jnp.left_shift(child, level)]
        which = jnp.where(jnp.bitwise_and(child, 1) == 1, plain, flipped)
        work_ref[level - 2] = system(which, pk_ref[OWN_TILE[level]], level % 2 == 0, rank, scale_of(level))
    eliminate(work_ref, 5)
    x_ref[...] = x_in_ref[...]
    for level in range(2, 7):
        child = jnp.right_shift(leaf, level - 1)
        rank = ranks_ref[level, jnp.left_shift(jnp.bitwise_xor(child, 1), level)]
        weight = solved(work_ref, level - 2, rank, scale_of(level))
        if level % 2 == 0:
            weight = pltpu.roll(weight, R, 1)
        group = (level - 1) // 2
        value = pair(x_ref[:, group * 128:group * 128 + 128])
        low_half, high_half = packed(value, weight, 0), packed(value, weight, 1)
        keep_ref[level - 2] = jnp.where(core == 0, low_half, high_half)
        send_ref[level - 2] = jnp.where(core == 0, high_half, low_half)
        for tile, target in ONWARD[level]:
            onward = dot_high(weight, pk_ref[tile], TN)
            x_ref[:, target * 128:target * 128 + 128] -= apply_nn(value, onward)


def late(ranks, coupling, near, far, x):
    return pl.pallas_call(
        late_kernel,
        out_shape=(shape(5, 128, 128), shape(5, 128, 128)),
        in_specs=[SMEM] + [VMEM] * 4,
        out_specs=(VMEM,) * 2,
        scratch_shapes=[
            pltpu.VMEM((9, R, 128), F32), pltpu.VMEM((COLS, UP), F32), pltpu.VMEM((5, R, 128), F32),
        ],
        compiler_params=params(20),
        cost_estimate=cost(4e9, 4e6),
        name="late",
    )(ranks, coupling, near, far, x)


def spot(index, size):
    return pl.ds(pl.multiple_of(index * size, size), size)


def deal_kernel(keep_ref, recv_ref, *refs):
    outs, own_ref, sum_ref = refs[:7], refs[7], refs[8]
    z = jnp.bitwise_and(jnp.right_shift(lax.axis_index("leaf"), 1), 7)
    sum_ref[...] = keep_ref[...] + recv_ref[...]
    outs[0][0:128] = sum_ref[0]
    for offset in range(1, 8):
        target = jnp.bitwise_xor(z, offset)
        out, at = outs[offset - 1], 128
        if offset in (2, 3):
            out[0:64], at = sum_ref[1, spot(jnp.bitwise_and(target, 1), 64), :], 64
        elif offset > 3:
            out[0:32], at = sum_ref[2, spot(jnp.bitwise_and(target, 3), 32), :], 32
        out[at:at + 16] = sum_ref[3, spot(target, 16), :]
        out[at + 16:at + 32] = sum_ref[4, spot(target, 16), :]
    own_ref[0:16] = sum_ref[3, spot(z, 16), :]
    own_ref[16:32] = sum_ref[4, spot(z, 16), :]


HEAD = (0, 128, 64, 64, 32, 32, 32, 32)


def deal(keep, recv):
    return pl.pallas_call(
        deal_kernel,
        out_shape=tuple(shape(HEAD[k] + 32, 128) for k in range(1, 8)) + (shape(32, 128),),
        in_specs=[VMEM] * 2,
        out_specs=(VMEM,) * 8,
        scratch_shapes=[pltpu.VMEM((5, 128, 128), F32)],
        compiler_params=params(6),
        cost_estimate=cost(1e8, 1e6),
        name="deal",
    )(keep, recv)


def gather_kernel(own_ref, *refs):
    got, (v3_ref, v4_ref, s5_ref, s6_ref) = refs[:7], refs[7:]
    total = own_ref[...]
    for offset in range(1, 8):
        at = HEAD[offset]
        total = total + got[offset - 1][at:at + 32]
    s5_ref[...] = total[0:16]
    s6_ref[...] = total[16:32]
    v3_ref[...] = got[1][0:64] + got[2][0:64]
    v4_ref[...] = (got[3][0:32] + got[4][0:32]) + (got[5][0:32] + got[6][0:32])


def gather(own, got):
    return pl.pallas_call(
        gather_kernel,
        out_shape=(shape(64, 128), shape(32, 128), shape(16, 128), shape(16, 128)),
        in_specs=[VMEM] * 8,
        out_specs=(VMEM,) * 4,
        compiler_params=params(6),
        cost_estimate=cost(1e8, 1e6),
        name="collect",
    )(own, *got)


def place_kernel(u2_ref, v3_ref, a3_ref, v4_ref, *refs):
    b4, v56_ref, w56, out_ref = refs[:3], refs[3], refs[4:11], refs[11]
    z = jnp.bitwise_and(jnp.right_shift(lax.axis_index("leaf"), 1), 7)
    out_ref[0] = u2_ref[0:128]
    out_ref[1, spot(jnp.bitwise_and(z, 1), 64), :] = v3_ref[...]
    out_ref[1, spot(1 - jnp.bitwise_and(z, 1), 64), :] = a3_ref[...]
    for offset, source in enumerate((v4_ref,) + tuple(b4)):
        out_ref[2, spot(jnp.bitwise_xor(jnp.bitwise_and(z, 3), offset), 32), :] = source[...]
    for offset, source in enumerate((v56_ref,) + tuple(w56)):
        where = spot(jnp.bitwise_xor(z, offset), 16)
        out_ref[3, where, :] = source[0:16]
        out_ref[4, where, :] = source[16:32]


def place(u2, v3, a3, v4, b4, v56, w56):
    return pl.pallas_call(
        place_kernel,
        out_shape=shape(5, 128, 128),
        in_specs=[VMEM] * 15,
        out_specs=VMEM,
        compiler_params=params(6),
        cost_estimate=cost(1e8, 1e6),
        name="place",
    )(u2, v3, a3, v4, *b4, v56, *w56)


def final_kernel(field_ref, bases_ref, u0_ref, u1_ref, near_ref, far_ref, out_ref, left_ref, all_ref):
    step = pl.program_id(0)
    half = step // (LEAF // BLK)

    @pl.when(step == 0)
    def _():
        core = jnp.bitwise_and(lax.axis_index("leaf"), 1)
        lane = lanes(128)

        def unpack(first, second, start, group):
            begin = pl.multiple_of(start * 256, 256)
            columns = slice(group * 128, group * 128 + 128)
            all_ref[pl.ds(begin, 128), columns] = jnp.where(lane < R, first, pltpu.roll(second, R, 1))
            all_ref[pl.ds(begin + 128, 128), columns] = jnp.where(lane < R, pltpu.roll(first, R, 1), second)

        for source, start in ((near_ref, core), (far_ref, 1 - core)):
            unpack(u1_ref[start], source[0], start, 0)
            unpack(source[1], source[2], start, 1)
            unpack(source[3], source[4], start, 2)
        high, low = split(all_ref[...])
        left_ref[:, 0:UP] = high
        left_ref[:, UP:2 * UP] = low
        high, low = split(u0_ref[...])
        left_ref[:, 2 * UP:2 * UP + 128] = high
        left_ref[:, 2 * UP + 128:2 * UP + 256] = low

    upper = bases_ref[1:].reshape(UP, BLK)
    base0 = bases_ref[0]
    nothing = jnp.zeros_like(base0)
    lower = jnp.concatenate(
        [jnp.where(half == 0, base0, nothing), jnp.where(half == 0, nothing, base0)], axis=0
    )
    right = jnp.concatenate([upper, upper, lower, lower], axis=0)
    out_ref[...] = field_ref[...] - dot(left_ref[...], right, NN)


def final(field, bases, u0, u1, near, far):
    whole = [pl.BlockSpec(a.shape, functools.partial(lambda n, j: (0,) * n, a.ndim)) for a in (u0, u1, near, far)]
    return pl.pallas_call(
        final_kernel,
        grid=(ROWS // BLK,),
        out_shape=shape(COLS, ROWS),
        in_specs=[
            pl.BlockSpec((COLS, BLK), lambda j: (0, j)),
            pl.BlockSpec((LEVELS, R, BLK), lambda j: (0, 0, j)),
        ] + whole,
        out_specs=pl.BlockSpec((COLS, BLK), lambda j: (0, j)),
        scratch_shapes=[pltpu.VMEM((COLS, 1024), BF16), pltpu.VMEM((COLS, UP), F32)],
        compiler_params=params(20),
        cost_estimate=cost(2 * COLS * 1024 * ROWS, 12e6),
        name="final",
    )(field, bases, u0, u1, near, far)


def swap(array, mask, axis="leaf"):
    return lax.ppermute(array, axis, [(i, i ^ mask) for i in range(lax.axis_size(axis))])


def local(samples, order_perm, leaf_factor, bases, coupling, ranks):
    leaf, col = lax.axis_index("leaf"), lax.axis_index("cols")
    core = leaf % 2
    tiles, own1, gram0, cross0 = grams(bases)
    sib1 = swap(own1, 1)
    mine = lax.dynamic_index_in_dim(tiles, core * 4 + col, 0, keepdims=False)
    theirs = lax.dynamic_index_in_dim(tiles, (1 - core) * 4 + col, 0, keepdims=False)
    permuted = permute(samples, order_perm.reshape(1, ROWS))
    field, q0, q = leaf_project(permuted, leaf_factor, bases)

    chip = (mine + swap(theirs, 1))[3:]
    got = swap(chip, 2)
    low_lane = lax.broadcasted_iota(jnp.int32, (8, 128), 1) < R
    pack = [chip[0], got[1], got[2]]
    total = chip[3:] + got[3:]
    got = swap(total, 4)
    pack += [jnp.where(low_lane, total[0], got[0]), got[1]]
    total = total[2:] + got[2:]
    got = swap(total, 8)
    pack += [total[0], got[1]]
    total = total[2:] + got[2:]
    got = swap(total, 16)
    pack += [jnp.where(low_lane, total[0], got[0]), total[1] + got[1]]
    pack = jnp.stack(pack)
    near = jnp.stack([pack] + [swap(pack, k, "cols") for k in (1, 2, 3)])
    far = swap(near, 1)

    u0, u1, x = early(ranks, coupling, gram0, cross0, own1, sib1, q0, q)
    u1 = swap(u1, 1)
    keep, send = late(ranks, coupling, near, far, x)
    dealt = deal(keep, swap(send, 1))
    got = [swap(dealt[k - 1], 2 * k) for k in range(1, 8)]
    v3, v4, s5, s6 = gather(dealt[7], got)
    a3 = swap(v3, 2)
    b4 = [swap(v4, 2 * k) for k in (1, 2, 3)]
    v56 = jnp.concatenate([swap(s5, 16), swap(s6, 32) + swap(s6, 48)], axis=0)
    w56 = [swap(v56, 2 * k) for k in range(1, 8)]
    near_u = place(got[0], v3, a3, v4, b4, v56, w56)
    far_u = swap(near_u, 1)
    return final(field, bases, u0, u1, near_u, far_u)


def solution(mesh):
    in_specs = (
        P("cols", "leaf"),
        P("leaf"),
        P("leaf", None, None),
        P(None, None, "leaf"),
        P(None, "leaf", None, None),
        P(),
    )
    out_specs = P("cols", "leaf")
    return jax.shard_map(local, mesh=mesh, in_specs=in_specs, out_specs=out_specs, check_vma=False)
```

```python
import functools
import math

import jax
import jax.numpy as jnp
from jax import lax
from jax.experimental import pallas as pl
from jax.experimental.pallas import tpu as pltpu
from jax.sharding import PartitionSpec as P


F32, BF16 = jnp.float32, jnp.bfloat16
HIGH = lax.Precision.HIGHEST
NT = (((1,), (1,)), ((), ()))
NN = (((1,), (0,)), ((), ()))
TN = (((0,), (0,)), ((), ()))

LEAF, R, ROWS, COLS, LEVELS = 1024, 64, 2048, 512, 7
UP = (LEVELS - 1) * R
BLK = 256
MIB = 1024 * 1024
VMEM = pl.BlockSpec(memory_space=pltpu.VMEM)
SMEM = pl.BlockSpec(memory_space=pltpu.SMEM)
HBM = pl.BlockSpec(memory_space=pltpu.HBM)


def params(mib, **more):
    return pltpu.CompilerParams(vmem_limit_bytes=mib * MIB, **more)


def cost(flops, moved):
    return pl.CostEstimate(flops=int(flops), bytes_accessed=int(moved), transcendentals=0)


def shape(*dims, dtype=F32):
    return jax.ShapeDtypeStruct(dims, dtype)


def stay(array):
    return pltpu.with_memory_space_constraint(array, pltpu.HBM)


def split(value):
    high = value.astype(BF16)
    return high, (value - high.astype(F32)).astype(BF16)


def dot(left, right, dims):
    return lax.dot_general(left, right, dims, preferred_element_type=F32)


def dot_high(left, right, dims):
    return lax.dot_general(left, right, dims, precision=HIGH, preferred_element_type=F32)


def twice(value, axis):
    return jnp.concatenate([value, value], axis=axis)


def gram_kernel(bases_ref, samples_ref, wide_ref, mine_ref, theirs_ref, first_ref, gram0_ref, cross0_ref, kept_ref,
                held_ref, tiles_ref, sems):
    load = pltpu.make_async_copy(bases_ref, held_ref, sems.at[0])
    load.start()
    keep = pltpu.make_async_copy(samples_ref, kept_ref, sems.at[1])
    keep.start()
    load.wait()
    nothing = jnp.zeros((R, LEAF), BF16)
    wide_ref[0:UP] = held_ref[1:].reshape(UP, ROWS)
    wide_ref[UP:UP + R, 0:LEAF] = held_ref[0, :, 0:LEAF]
    wide_ref[UP:UP + R, LEAF:] = nothing
    wide_ref[UP + R:, 0:LEAF] = nothing
    wide_ref[UP + R:, LEAF:] = held_ref[0, :, LEAF:]
    wide = wide_ref[...]
    gram = dot(wide, wide, NT)
    first_ref[...] = gram[:R, :UP]
    for part in range(8):
        tile = 0
        for level in range(6):
            top = level * R + 8 * part
            for lane in range(level // 2, 3):
                tiles_ref[part, tile] = gram[top:top + 8, lane * 128:lane * 128 + 128]
                tile += 1
    part, other = lax.axis_index("cols"), lax.axis_index("core") * 4
    mine_ref[...] = tiles_ref[part + other]
    theirs_ref[...] = tiles_ref[part + 4 - other]
    gram0_ref[...] = gram[UP:, UP:]
    cross0_ref[...] = gram[UP:, :UP]
    keep.wait()


def grams(bases, samples):
    return pl.pallas_call(
        gram_kernel,
        out_shape=(
            shape(512, ROWS, dtype=BF16), shape(12, 8, 128), shape(12, 8, 128), shape(R, UP), shape(128, 128),
            shape(128, UP),
            pltpu.VMEM((COLS, ROWS), BF16),
        ),
        in_specs=[HBM] * 2,
        out_specs=(VMEM,) * 7,
        scratch_shapes=[pltpu.VMEM((LEVELS, R, ROWS), BF16), pltpu.VMEM((8, 12, 8, 128), F32), pltpu.SemaphoreType.DMA((2,))],
        compiler_params=params(14),
        cost_estimate=cost(2e9, 4e6),
        name="gram",
    )(stay(bases), stay(samples))


def permute_block(samples_ref, order_ref, out_ref, begin):
    def block(j, carry):
        columns = pl.ds(pl.multiple_of(j * BLK, BLK), BLK)
        rows = lax.broadcasted_iota(jnp.int32, (ROWS, BLK), 0)
        source = pl.ds(pl.multiple_of(begin + j * BLK, BLK), BLK)
        local = jnp.bitwise_and(order_ref[:, source], ROWS - 1)
        chosen = (rows == local).astype(F32).astype(BF16)
        out_ref[:, columns] = dot(samples_ref[...], chosen, NN).astype(BF16)
        return carry

    lax.fori_loop(0, LEAF // BLK, block, 0)


def permute_first_kernel(samples_ref, order_ref, factor_ref, out_ref, kept_ref, sem):
    keep = pltpu.make_async_copy(factor_ref, kept_ref, sem)
    keep.start()
    permute_block(samples_ref, order_ref, out_ref, 0)
    keep.wait()


def permute_second_kernel(samples_ref, order_ref, out_ref):
    permute_block(samples_ref, order_ref, out_ref, LEAF)


def permute_first(samples, order, factor):
    return pl.pallas_call(
        permute_first_kernel,
        out_shape=(shape(COLS, LEAF, dtype=BF16), pltpu.VMEM((2, LEAF, LEAF), BF16)),
        in_specs=[VMEM, VMEM, HBM],
        out_specs=(VMEM,) * 2,
        scratch_shapes=[pltpu.SemaphoreType.DMA],
        compiler_params=params(14),
        cost_estimate=cost(COLS * ROWS * ROWS, 4e6),
        name="permute_first",
    )(samples, order, stay(factor))


def permute_second(samples, order):
    return pl.pallas_call(
        permute_second_kernel,
        out_shape=shape(COLS, LEAF, dtype=BF16),
        in_specs=[VMEM, VMEM],
        out_specs=VMEM,
        compiler_params=params(10),
        cost_estimate=cost(COLS * ROWS * ROWS, 4e6),
        name="permute_second",
    )(samples, order)


def leaf_kernel(permuted_ref, factor_ref, field_ref, *, half):
    def block(j, carry):
        columns = pl.ds(pl.multiple_of(j * 512, 512), 512)
        field_ref[:, columns] = dot(permuted_ref[...], factor_ref[half, :, columns], NN)
        return carry

    lax.fori_loop(0, 2, block, 0)


def leaf_product(permuted, factor, half):
    return pl.pallas_call(
        functools.partial(leaf_kernel, half=half),
        out_shape=shape(COLS, LEAF),
        in_specs=[VMEM] * 2,
        out_specs=VMEM,
        compiler_params=params(12),
        cost_estimate=cost(2 * COLS * LEAF * LEAF, 5e6),
    )(permuted, factor)


def project_kernel(first_ref, second_ref, wide_ref, q_ref):
    def rows_of(i, carry):
        rows = pl.ds(pl.multiple_of(i * 256, 256), 256)
        total = None
        for half, source in enumerate((first_ref, second_ref)):
            for part in split(source[rows, :]):
                term = dot(part, wide_ref[:, half * LEAF:(half + 1) * LEAF], NT)
                total = term if total is None else total + term
        q_ref[rows, :] = total
        return carry

    lax.fori_loop(0, COLS // 256, rows_of, 0)


def project(first, second, wide):
    return pl.pallas_call(
        project_kernel,
        out_shape=shape(COLS, 512),
        in_specs=[VMEM] * 3,
        out_specs=VMEM,
        compiler_params=params(14),
        cost_estimate=cost(4 * COLS * 512 * ROWS, 7e6),
        name="project",
    )(first, second, wide)


def coupling_forms(link):
    flipped = link.T
    plain = twice(flipped, 0).T
    return plain, twice(link, 0).T


def lanes(rows=R):
    return lax.broadcasted_iota(jnp.int32, (rows, 128), 1)


def system(link_dup, gram_tile, upper_half, rank_own, scale):
    lane = lanes()
    joint = jnp.where(jnp.bitwise_and(lane, R - 1) < rank_own, link_dup * scale, 0.0)
    placed = jnp.where((lane >= R) == upper_half, joint, 0.0)
    inner = dot_high(gram_tile, twice(placed, 0), NT)
    outer = dot_high(joint[:, :R], inner, NN)
    row = lax.broadcasted_iota(jnp.int32, (R, 128), 0)
    outer = outer + jnp.where(row == lane, 1.0, 0.0)
    return jnp.where(lane < R, outer, joint)


def eliminate(work_ref, count):
    row = lax.broadcasted_iota(jnp.int32, (count, R, 128), 1)
    tile_row = lax.broadcasted_iota(jnp.int32, (count, 8, 128), 1)

    def block(step, carry):
        top = pl.multiple_of(step * 8, 8)
        here = (row >= top) & (row < top + 8)
        value = work_ref[...]
        tile = work_ref[:, pl.ds(top, 8), :]
        heads = [jnp.broadcast_to(tile[:, :, j:j + 1], (count, 8, 128)) for j in range(8)]
        columns = [jnp.broadcast_to(value[:, :, j:j + 1], (count, R, 128)) for j in range(8)]
        for j in range(8):
            inverse = 1.0 / heads[j][:, j:j + 1, :]
            pivot = tile[:, j:j + 1, :] * inverse
            tile = jnp.where(tile_row == j, pivot, tile - heads[j] * pivot)
            for i in range(j + 1, 8):
                element = heads[i][:, j:j + 1, :] * inverse
                heads[i] = jnp.where(tile_row == j, element, heads[i] - heads[j] * element)
        for j in range(8):
            value = value - columns[j] * tile[:, j:j + 1, :]
        value = jnp.where(here, jnp.concatenate([tile] * 8, axis=1), value)
        work_ref[...] = pltpu.roll(value, 120, 2)
        return carry

    lax.fori_loop(0, 8, block, 0)


def solved(work_ref, item, rank_sibling, scale):
    row = lax.broadcasted_iota(jnp.int32, (R, 128), 0)
    keep = (row < rank_sibling) & (lanes() < R)
    return jnp.where(keep, work_ref[item] * scale, 0.0)


def pair(value):
    high, low = split(value)
    return jnp.concatenate([high, low], axis=1)


def apply_nt(value_pair, weight):
    high, low = split(weight)
    return dot(value_pair, twice(high, 1), NT) + dot(value_pair, twice(low, 1), NT)


def apply_nn(value_pair, weight):
    high, low = split(weight)
    return dot(value_pair, twice(high, 0), NN) + dot(value_pair, twice(low, 0), NN)


def packed(value_pair, weight):
    nothing = jnp.zeros_like(weight)
    left = jnp.concatenate([value_pair[0:128], value_pair[256:384]], axis=0)
    right = jnp.concatenate([value_pair[128:256], value_pair[384:512]], axis=0)
    return apply_nt(left, jnp.concatenate([weight, nothing], 0)) + apply_nt(right, jnp.concatenate([nothing, weight], 0))


def leaf_index():
    return (lax.axis_index("x") * 8 + lax.axis_index("z")) * 2 + lax.axis_index("core")


def scale_of(level):
    return 1.0 / math.sqrt(LEAF * 2**level)


def solve_early_kernel(ranks_ref, link_ref, gram0_ref, own1_ref, sib1_ref, from0_ref, weight_ref, onward_ref, work_ref):
    leaf = leaf_index()
    second = lax.axis_index("core")
    plain0, flipped0 = coupling_forms(link_ref[0, 0])
    plain1, flipped1 = coupling_forms(link_ref[1, 0])
    rank_f, rank_s = ranks_ref[0, 2 * leaf], ranks_ref[0, 2 * leaf + 1]
    rank_1, rank_1s = ranks_ref[1, 2 * leaf], ranks_ref[1, 2 * jnp.bitwise_xor(leaf, 1)]
    scale0, scale1 = scale_of(0), scale_of(1)
    work_ref[0] = system(flipped0, gram0_ref[0:R], False, rank_f, scale0)
    work_ref[1] = system(plain0, gram0_ref[R:], True, rank_s, scale0)
    work_ref[2] = system(jnp.where(second == 1, plain1, flipped1), own1_ref[:, :128], False, rank_1, scale1)
    eliminate(work_ref, 3)
    from0_ref[R:] = solved(work_ref, 0, rank_s, scale0)
    from0_ref[0:R] = pltpu.roll(solved(work_ref, 1, rank_f, scale0), R, 1)
    weight = solved(work_ref, 2, rank_1s, scale1)
    weight_ref[...] = weight
    onward_ref[...] = dot_high(weight, sib1_ref[...], TN)


def solve_early(ranks, coupling, gram0, own1, sib1):
    return pl.pallas_call(
        solve_early_kernel,
        out_shape=(shape(128, 128), shape(R, 128), shape(128, UP)),
        in_specs=[SMEM] + [VMEM] * 4,
        out_specs=(VMEM,) * 3,
        scratch_shapes=[pltpu.VMEM((3, R, 128), F32)],
        compiler_params=params(8),
        cost_estimate=cost(3e9, 4e6),
        name="solve_early",
    )(ranks, coupling, gram0, own1, sib1)


def early_kernel(q_ref, from0_ref, cross0_ref, weight_ref, onward_ref, u0_ref, u1_ref, x_ref):
    u0 = apply_nt(pair(q_ref[:, UP:]), from0_ref[...])
    u0_ref[...] = u0
    zero = pair(u0)
    cross0 = cross0_ref[...]
    head = pair(q_ref[:, :128] - apply_nn(zero, cross0[:, :128]))
    both = packed(head, weight_ref[...])
    u1_ref[0] = both[:128]
    u1_ref[1] = both[128:]
    onward = onward_ref[...]
    for group in range(3):
        at = slice(group * 128, group * 128 + 128)
        x_ref[:, at] = q_ref[:, at] - apply_nn(zero, cross0[:, at]) - apply_nn(head, onward[:, at])


def early(q, from0, cross0, weight, onward):
    return pl.pallas_call(
        early_kernel,
        out_shape=(shape(COLS, 128), shape(2, 128, 128), shape(COLS, UP)),
        in_specs=[VMEM] * 5,
        out_specs=(VMEM,) * 3,
        compiler_params=params(12),
        cost_estimate=cost(3e9, 4e6),
        name="early",
    )(q, from0, cross0, weight, onward)


OWN_TILE = {2: 0, 3: 3, 4: 5, 5: 7, 6: 8}
ONWARD = {2: ((1, 1), (2, 2)), 3: ((3, 1), (4, 2)), 4: ((6, 2),), 5: ((7, 2),), 6: ()}


def late_kernel(ranks_ref, link_ref, near_ref, far_ref, x_ref, keep_ref, send_ref, pk_ref, work_ref):
    leaf, col, core = leaf_index(), lax.axis_index("cols"), lax.axis_index("core")
    for other, source in ((0, near_ref), (1, far_ref)):
        for slot, offset in enumerate((0, 1, 3, 2)):
            part = jnp.bitwise_xor(core, other) * 4 + jnp.bitwise_xor(col, offset)
            rows = pl.ds(pl.multiple_of(part * 8, 8), 8)
            for tile in range(9):
                pk_ref[tile, rows, :] = source[slot, tile]
    systems = []
    for level in range(2, 7):
        child = jnp.right_shift(leaf, level - 1)
        plain, flipped = coupling_forms(link_ref[level, 0])
        rank = ranks_ref[level, jnp.left_shift(child, level)]
        which = jnp.where(jnp.bitwise_and(child, 1) == 1, plain, flipped)
        systems.append(system(which, pk_ref[OWN_TILE[level]], level % 2 == 0, rank, scale_of(level)))
    for item in range(5):
        work_ref[item] = systems[item]
    eliminate(work_ref, 5)
    weights, onwards = {}, {}
    for level in range(2, 7):
        child = jnp.right_shift(leaf, level - 1)
        rank = ranks_ref[level, jnp.left_shift(jnp.bitwise_xor(child, 1), level)]
        weight = solved(work_ref, level - 2, rank, scale_of(level))
        if level % 2 == 0:
            weight = pltpu.roll(weight, R, 1)
        weights[level] = weight
        onwards[level] = [(dot_high(weight, pk_ref[tile], TN), target) for tile, target in ONWARD[level]]
    groups = [x_ref[:, g * 128:g * 128 + 128] for g in range(3)]
    for level in range(2, 7):
        value = pair(groups[(level - 1) // 2])
        for onward, target in onwards[level]:
            groups[target] = groups[target] - apply_nn(value, onward)
        both = packed(value, weights[level])
        keep_ref[level - 2] = jnp.where(core == 0, both[:128], both[128:])
        send_ref[level - 2] = jnp.where(core == 0, both[128:], both[:128])


def late(ranks, coupling, near, far, x):
    return pl.pallas_call(
        late_kernel,
        out_shape=(shape(5, 128, 128), shape(5, 128, 128)),
        in_specs=[SMEM] + [VMEM] * 4,
        out_specs=(VMEM,) * 2,
        scratch_shapes=[pltpu.VMEM((9, R, 128), F32), pltpu.VMEM((5, R, 128), F32)],
        compiler_params=params(16),
        cost_estimate=cost(4e9, 4e6),
        name="late",
    )(ranks, coupling, near, far, x)


def turned(value):
    return pltpu.roll(value, 4, 0)


def two_kernel(keep_ref, recv_ref, two_ref):
    two_ref[...] = keep_ref[0] + recv_ref[0]


def level_two(keep, recv):
    return pl.pallas_call(
        two_kernel,
        out_shape=shape(128, 128),
        in_specs=[VMEM] * 2,
        out_specs=VMEM,
        compiler_params=params(4),
        cost_estimate=cost(1e6, 1e5),
        name="two",
    )(keep, recv)


def deal_kernel(keep_ref, recv_ref, out_ref):
    top = lax.broadcasted_iota(jnp.int32, (8, 128), 0) < 4
    for t in range(16):
        rows = slice(8 * t, 8 * t + 8)
        for group in range(2):
            first = keep_ref[2 * group + 1, rows] + recv_ref[2 * group + 1, rows]
            second = keep_ref[2 * group + 2, rows] + recv_ref[2 * group + 2, rows]
            to = slice(8 * group, 8 * group + 8)
            out_ref[2 * t, to] = jnp.where(top, first, turned(second))
            out_ref[2 * t + 1, to] = jnp.where(top, turned(first), second)


def deal(keep, recv):
    return pl.pallas_call(
        deal_kernel,
        out_shape=shape(32, 16, 128),
        in_specs=[VMEM] * 2,
        out_specs=VMEM,
        compiler_params=params(4),
        cost_estimate=cost(1e8, 1e6),
        name="deal",
    )(keep, recv)


def collect_kernel(got_ref, out_ref):
    top = lax.broadcasted_iota(jnp.int32, (8, 128), 0) < 4
    pieces = [got_ref[q] for q in range(32)]
    sums = []
    for _ in range(4):
        pieces = [pieces[2 * c] + pieces[2 * c + 1] for c in range(len(pieces) // 2)]
        sums.append(pieces)
    for e in range(32):
        parts = [sums[k][(e >> (k + 1)) ^ 1] for k in range(4)]
        out_ref[e, 0:8] = jnp.where(top, parts[0][0:8], parts[1][0:8])
        out_ref[e, 8:16] = jnp.where(top, parts[2][8:16], parts[3][8:16])


def collect(got):
    return pl.pallas_call(
        collect_kernel,
        out_shape=shape(32, 16, 128),
        in_specs=[VMEM],
        out_specs=VMEM,
        compiler_params=params(4),
        cost_estimate=cost(1e8, 1e6),
        name="collect",
    )(got)


def final_kernel(field0_ref, field1_ref, wide_ref, u0_ref, u1_ref, near2_ref, far2_ref, near_ref, far_ref,
                 out_ref, left_ref, all_ref):
    step = pl.program_id(0)
    half = step // (LEAF // BLK)

    @pl.when(step == 0)
    def _():
        core = lax.axis_index("core")
        top = lax.broadcasted_iota(jnp.int32, (8, 128), 0) < 4
        lane = lanes(8)

        def unpack(first, second, begin, group):
            columns = slice(group * 128, group * 128 + 128)
            upper = pl.ds(pl.multiple_of(begin, 8), 8)
            lower = pl.ds(pl.multiple_of(begin + 128, 8), 8)
            all_ref[upper, columns] = jnp.where(lane < R, first, pltpu.roll(second, R, 1))
            all_ref[lower, columns] = jnp.where(lane < R, pltpu.roll(first, R, 1), second)

        for two, rest, start in ((near2_ref, near_ref, core), (far2_ref, far_ref, 1 - core)):
            for t in range(16):
                rows = slice(8 * t, 8 * t + 8)
                begin = start * 256 + 8 * t
                unpack(u1_ref[start, rows], two[rows], begin, 0)
                for group in range(2):
                    one = rest[2 * t, 8 * group:8 * group + 8]
                    other = rest[2 * t + 1, 8 * group:8 * group + 8]
                    unpack(
                        jnp.where(top, one, turned(other)), jnp.where(top, turned(one), other), begin, group + 1
                    )
        high, low = split(all_ref[...])
        left_ref[:, 0:UP] = high
        left_ref[:, 512:512 + UP] = low
        high, low = split(u0_ref[...])
        left_ref[:, UP:512] = high
        left_ref[:, 512 + UP:] = low

    right = wide_ref[...]
    update = dot(left_ref[:, :512], right, NN) + dot(left_ref[:, 512:], right, NN)

    @pl.when(half == 0)
    def _():
        out_ref[...] = field0_ref[...] - update

    @pl.when(half == 1)
    def _():
        out_ref[...] = field1_ref[...] - update


def final(field0, field1, wide, *updates):
    steps = LEAF // BLK
    return pl.pallas_call(
        final_kernel,
        grid=(ROWS // BLK,),
        out_shape=shape(COLS, ROWS),
        in_specs=[
            pl.BlockSpec((COLS, BLK), lambda j: (0, jnp.minimum(j, steps - 1))),
            pl.BlockSpec((COLS, BLK), lambda j: (0, jnp.maximum(j - steps, 0))),
            pl.BlockSpec((512, BLK), lambda j: (0, j)),
        ] + [VMEM] * 6,
        out_specs=pl.BlockSpec((COLS, BLK), lambda j: (0, j)),
        scratch_shapes=[pltpu.VMEM((COLS, 1024), BF16), pltpu.VMEM((COLS, UP), F32)],
        compiler_params=params(16),
        cost_estimate=cost(2 * COLS * 1024 * ROWS, 12e6),
        name="final",
    )(stay(field0), stay(field1), stay(wide), *updates)


def swap(array, mask, axis):
    return lax.ppermute(array, axis, [(i, i ^ mask) for i in range(lax.axis_size(axis))])


def local(samples, order_perm, leaf_factor, bases, coupling, ranks):
    wide, mine, theirs, own1, gram0, cross0, samples = grams(bases, samples)
    order = order_perm.reshape(1, ROWS)
    got = swap(theirs, 1, "core")
    sib1 = swap(own1, 1, "core")
    permuted0, factor = permute_first(samples, order, leaf_factor)
    permuted1 = permute_second(samples, order)
    field0 = leaf_product(permuted0, factor, 0)
    field1 = leaf_product(permuted1, factor, 1)
    q = project(field0, field1, wide)
    from0, weight1, onward1 = solve_early(ranks, coupling, gram0, own1, sib1)
    u0, u1, x = early(q, from0, cross0, weight1, onward1)

    chip = (mine + got)[3:]
    got = swap(chip, 1, "z")
    low_lane = lax.broadcasted_iota(jnp.int32, (8, 128), 1) < R
    pack = [chip[0], got[1], got[2]]
    total = chip[3:] + got[3:]
    got = swap(total, 2, "z")
    pack += [jnp.where(low_lane, total[0], got[0]), got[1]]
    total = total[2:] + got[2:]
    got = swap(total, 4, "z")
    pack += [total[0], got[1]]
    total = total[2:] + got[2:]
    got = swap(total, 1, "x")
    pack += [jnp.where(low_lane, total[0], got[0]), total[1] + got[1]]
    pack = jnp.stack(pack)
    got = swap(pack, 1, "cols")
    pack = jnp.stack([pack, got])
    got = swap(pack, 3, "cols")
    near = jnp.concatenate([pack, got], axis=0)
    far = swap(near, 1, "core")
    u1 = swap(u1, 1, "core")
    keep, send = late(ranks, coupling, near, far, x)
    got = swap(send, 1, "core")
    two = level_two(keep, got)
    two = swap(two, 1, "z")
    dealt = deal(keep, got)
    got = lax.all_to_all(dealt, ("x", "z"), 0, 0, tiled=True)
    far_two = swap(two, 1, "core")
    total = collect(got)
    back = lax.all_to_all(total, ("x", "z"), 0, 0, tiled=True)
    far_back = swap(back, 1, "core")
    return final(field0, field1, wide, u0, u1, two, far_two, back, far_back)


def solution(mesh):
    fine = jax.sharding.Mesh(mesh.devices.reshape(4, 8, 2, 4), ("x", "z", "core", "cols"))
    leaf = ("x", "z", "core")
    in_specs = (
        P("cols", leaf),
        P(leaf),
        P(leaf, None, None),
        P(None, None, leaf),
        P(None, leaf, None, None),
        P(),
    )
    out_specs = P("cols", leaf)
    return jax.shard_map(local, mesh=fine, in_specs=in_specs, out_specs=out_specs, check_vma=False)
```

```python
import functools
import math

import jax
import jax.numpy as jnp
from jax import lax
from jax.experimental import pallas as pl
from jax.experimental.pallas import tpu as pltpu
from jax.sharding import PartitionSpec as P


F32, BF16 = jnp.float32, jnp.bfloat16
HIGH = lax.Precision.HIGHEST
NT = (((1,), (1,)), ((), ()))
NN = (((1,), (0,)), ((), ()))
TN = (((0,), (0,)), ((), ()))

LEAF, R, ROWS, COLS, LEVELS = 1024, 64, 2048, 512, 7
UP = (LEVELS - 1) * R
BLK = 256
MIB = 1024 * 1024
VMEM = pl.BlockSpec(memory_space=pltpu.VMEM)
SMEM = pl.BlockSpec(memory_space=pltpu.SMEM)
HBM = pl.BlockSpec(memory_space=pltpu.HBM)


def params(mib, **more):
    return pltpu.CompilerParams(vmem_limit_bytes=mib * MIB, **more)


def cost(flops, moved):
    return pl.CostEstimate(flops=int(flops), bytes_accessed=int(moved), transcendentals=0)


def shape(*dims, dtype=F32):
    return jax.ShapeDtypeStruct(dims, dtype)


def stay(array):
    return pltpu.with_memory_space_constraint(array, pltpu.HBM)


def split(value):
    high = value.astype(BF16)
    return high, (value - high.astype(F32)).astype(BF16)


def dot(left, right, dims):
    return lax.dot_general(left, right, dims, preferred_element_type=F32)


def dot_high(left, right, dims):
    return lax.dot_general(left, right, dims, precision=HIGH, preferred_element_type=F32)


def twice(value, axis):
    return jnp.concatenate([value, value], axis=axis)


def gram_kernel(bases_ref, samples_ref, wide_ref, mine_ref, theirs_ref, first_ref, gram0_ref, cross0_ref, kept_ref,
                held_ref, tiles_ref, sems):
    load = pltpu.make_async_copy(bases_ref, held_ref, sems.at[0])
    load.start()
    keep = pltpu.make_async_copy(samples_ref, kept_ref, sems.at[1])
    keep.start()
    load.wait()
    nothing = jnp.zeros((R, LEAF), BF16)
    wide_ref[0:UP] = held_ref[1:].reshape(UP, ROWS)
    wide_ref[UP:UP + R, 0:LEAF] = held_ref[0, :, 0:LEAF]
    wide_ref[UP:UP + R, LEAF:] = nothing
    wide_ref[UP + R:, 0:LEAF] = nothing
    wide_ref[UP + R:, LEAF:] = held_ref[0, :, LEAF:]
    wide = wide_ref[...]
    gram = dot(wide, wide, NT)
    first_ref[...] = gram[:R, :UP]
    for part in range(8):
        tile = 0
        for level in range(6):
            top = level * R + 8 * part
            for lane in range(level // 2, 3):
                tiles_ref[part, tile] = gram[top:top + 8, lane * 128:lane * 128 + 128]
                tile += 1
    part, other = lax.axis_index("cols"), lax.axis_index("core") * 4
    mine_ref[...] = tiles_ref[part + other]
    theirs_ref[...] = tiles_ref[part + 4 - other]
    gram0_ref[...] = gram[UP:, UP:]
    cross0_ref[...] = gram[UP:, :UP]
    keep.wait()


def grams(bases, samples):
    return pl.pallas_call(
        gram_kernel,
        out_shape=(
            shape(512, ROWS, dtype=BF16), shape(12, 8, 128), shape(12, 8, 128), shape(R, UP), shape(128, 128),
            shape(128, UP),
            pltpu.VMEM((COLS, ROWS), BF16),
        ),
        in_specs=[HBM] * 2,
        out_specs=(VMEM,) * 7,
        scratch_shapes=[pltpu.VMEM((LEVELS, R, ROWS), BF16), pltpu.VMEM((8, 12, 8, 128), F32), pltpu.SemaphoreType.DMA((2,))],
        compiler_params=params(14),
        cost_estimate=cost(2e9, 4e6),
        name="gram",
    )(stay(bases), stay(samples))


def permute_block(samples_ref, order_ref, out_ref, begin):
    def block(j, carry):
        columns = pl.ds(pl.multiple_of(j * BLK, BLK), BLK)
        rows = lax.broadcasted_iota(jnp.int32, (ROWS, BLK), 0)
        source = pl.ds(pl.multiple_of(begin + j * BLK, BLK), BLK)
        local = jnp.bitwise_and(order_ref[:, source], ROWS - 1)
        chosen = (rows == local).astype(F32).astype(BF16)
        out_ref[:, columns] = dot(samples_ref[...], chosen, NN).astype(BF16)
        return carry

    lax.fori_loop(0, LEAF // BLK, block, 0)


def permute_first_kernel(samples_ref, order_ref, factor_ref, out_ref, kept_ref, sem):
    keep = pltpu.make_async_copy(factor_ref, kept_ref, sem)
    keep.start()
    permute_block(samples_ref, order_ref, out_ref, 0)
    keep.wait()


def permute_second_kernel(samples_ref, order_ref, out_ref):
    permute_block(samples_ref, order_ref, out_ref, LEAF)


def permute_first(samples, order, factor):
    return pl.pallas_call(
        permute_first_kernel,
        out_shape=(shape(COLS, LEAF, dtype=BF16), pltpu.VMEM((2, LEAF, LEAF), BF16)),
        in_specs=[VMEM, VMEM, HBM],
        out_specs=(VMEM,) * 2,
        scratch_shapes=[pltpu.SemaphoreType.DMA],
        compiler_params=params(14),
        cost_estimate=cost(COLS * ROWS * ROWS, 4e6),
        name="permute_first",
    )(samples, order, stay(factor))


def permute_second(samples, order):
    return pl.pallas_call(
        permute_second_kernel,
        out_shape=shape(COLS, LEAF, dtype=BF16),
        in_specs=[VMEM, VMEM],
        out_specs=VMEM,
        compiler_params=params(10),
        cost_estimate=cost(COLS * ROWS * ROWS, 4e6),
        name="permute_second",
    )(samples, order)


def leaf_kernel(permuted_ref, factor_ref, field_ref, *, half):
    def block(j, carry):
        columns = pl.ds(pl.multiple_of(j * 512, 512), 512)
        field_ref[:, columns] = dot(permuted_ref[...], factor_ref[half, :, columns], NN)
        return carry

    lax.fori_loop(0, 2, block, 0)


def leaf_product(permuted, factor, half):
    return pl.pallas_call(
        functools.partial(leaf_kernel, half=half),
        out_shape=shape(COLS, LEAF),
        in_specs=[VMEM] * 2,
        out_specs=VMEM,
        compiler_params=params(12),
        cost_estimate=cost(2 * COLS * LEAF * LEAF, 5e6),
    )(permuted, factor)


def project_kernel(first_ref, second_ref, wide_ref, q_ref):
    def rows_of(i, carry):
        rows = pl.ds(pl.multiple_of(i * 256, 256), 256)
        total = None
        for half, source in enumerate((first_ref, second_ref)):
            for part in split(source[rows, :]):
                term = dot(part, wide_ref[:, half * LEAF:(half + 1) * LEAF], NT)
                total = term if total is None else total + term
        q_ref[rows, :] = total
        return carry

    lax.fori_loop(0, COLS // 256, rows_of, 0)


def project(first, second, wide):
    return pl.pallas_call(
        project_kernel,
        out_shape=shape(COLS, 512),
        in_specs=[VMEM] * 3,
        out_specs=VMEM,
        compiler_params=params(14),
        cost_estimate=cost(4 * COLS * 512 * ROWS, 7e6),
        name="project",
    )(first, second, wide)


def coupling_forms(link):
    flipped = link.T
    plain = twice(flipped, 0).T
    return plain, twice(link, 0).T


def lanes(rows=R):
    return lax.broadcasted_iota(jnp.int32, (rows, 128), 1)


def jointly(link_dup, rank_own, scale):
    return jnp.where(jnp.bitwise_and(lanes(), R - 1) < rank_own, link_dup * scale, 0.0)


def system(joint, gram_tile, upper_half):
    lane = lanes()
    placed = jnp.where((lane >= R) == upper_half, joint, 0.0)
    inner = dot_high(gram_tile, twice(placed, 0), NT)
    outer = dot_high(joint[:, :R], inner, NN)
    row = lax.broadcasted_iota(jnp.int32, (R, 128), 0)
    outer = outer + jnp.where(row == lane, 1.0, 0.0)
    return jnp.where(lane < R, outer, joint)


def eliminate(work_ref, count):
    row = lax.broadcasted_iota(jnp.int32, (count, R, 128), 1)
    tile_row = lax.broadcasted_iota(jnp.int32, (count, 8, 128), 1)

    def block(step, carry):
        top = pl.multiple_of(step * 8, 8)
        here = (row >= top) & (row < top + 8)
        value = work_ref[...]
        tile = work_ref[:, pl.ds(top, 8), :]
        heads = [jnp.broadcast_to(tile[:, :, j:j + 1], (count, 8, 128)) for j in range(8)]
        columns = [jnp.broadcast_to(value[:, :, j:j + 1], (count, R, 128)) for j in range(8)]
        for j in range(8):
            inverse = 1.0 / heads[j][:, j:j + 1, :]
            pivot = tile[:, j:j + 1, :] * inverse
            tile = jnp.where(tile_row == j, pivot, tile - heads[j] * pivot)
            for i in range(j + 1, 8):
                element = heads[i][:, j:j + 1, :] * inverse
                heads[i] = jnp.where(tile_row == j, element, heads[i] - heads[j] * element)
        for j in range(8):
            value = value - columns[j] * tile[:, j:j + 1, :]
        value = jnp.where(here, jnp.concatenate([tile] * 8, axis=1), value)
        work_ref[...] = pltpu.roll(value, 120, 2)
        return carry

    lax.fori_loop(0, 8, block, 0)


def solved(work_ref, item, rank_sibling, scale):
    row = lax.broadcasted_iota(jnp.int32, (R, 128), 0)
    keep = (row < rank_sibling) & (lanes() < R)
    return jnp.where(keep, work_ref[item] * scale, 0.0)


def pair(value):
    high, low = split(value)
    return jnp.concatenate([high, low], axis=1)


def apply_nt(value_pair, weight):
    high, low = split(weight)
    return dot(value_pair, twice(high, 1), NT) + dot(value_pair, twice(low, 1), NT)


def apply_nn(value_pair, weight):
    high, low = split(weight)
    return dot(value_pair, twice(high, 0), NN) + dot(value_pair, twice(low, 0), NN)


def packed(value_pair, weight):
    nothing = jnp.zeros_like(weight)
    left = jnp.concatenate([value_pair[0:128], value_pair[256:384]], axis=0)
    right = jnp.concatenate([value_pair[128:256], value_pair[384:512]], axis=0)
    return apply_nt(left, jnp.concatenate([weight, nothing], 0)) + apply_nt(right, jnp.concatenate([nothing, weight], 0))


def leaf_index():
    return (lax.axis_index("x") * 8 + lax.axis_index("z")) * 2 + lax.axis_index("core")


def scale_of(level):
    return 1.0 / math.sqrt(LEAF * 2**level)


def solve_early_kernel(ranks_ref, link_ref, gram0_ref, own1_ref, sib1_ref, from0_ref, weight_ref, onward_ref, work_ref):
    leaf = leaf_index()
    second = lax.axis_index("core")
    plain0, flipped0 = coupling_forms(link_ref[0, 0])
    plain1, flipped1 = coupling_forms(link_ref[1, 0])
    rank_f, rank_s = ranks_ref[0, 2 * leaf], ranks_ref[0, 2 * leaf + 1]
    rank_1, rank_1s = ranks_ref[1, 2 * leaf], ranks_ref[1, 2 * jnp.bitwise_xor(leaf, 1)]
    scale0, scale1 = scale_of(0), scale_of(1)
    work_ref[0] = system(jointly(flipped0, rank_f, scale0), gram0_ref[0:R], False)
    work_ref[1] = system(jointly(plain0, rank_s, scale0), gram0_ref[R:], True)
    joint1 = jointly(jnp.where(second == 1, plain1, flipped1), rank_1, scale1)
    work_ref[2] = system(joint1, own1_ref[:, :128], False)
    eliminate(work_ref, 3)
    from0_ref[R:] = solved(work_ref, 0, rank_s, scale0)
    from0_ref[0:R] = pltpu.roll(solved(work_ref, 1, rank_f, scale0), R, 1)
    weight = solved(work_ref, 2, rank_1s, scale1)
    weight_ref[...] = weight
    onward_ref[...] = dot_high(weight, sib1_ref[...], TN)


def solve_early(ranks, coupling, gram0, own1, sib1):
    return pl.pallas_call(
        solve_early_kernel,
        out_shape=(shape(128, 128), shape(R, 128), shape(128, UP)),
        in_specs=[SMEM] + [VMEM] * 4,
        out_specs=(VMEM,) * 3,
        scratch_shapes=[pltpu.VMEM((3, R, 128), F32)],
        compiler_params=params(8),
        cost_estimate=cost(3e9, 4e6),
        name="solve_early",
    )(ranks, coupling, gram0, own1, sib1)


def early_kernel(ranks_ref, link_ref, q_ref, from0_ref, cross0_ref, weight_ref, onward_ref,
                 u0_ref, u1_ref, x_ref, joint_ref):
    leaf = leaf_index()
    for level in range(2, 7):
        child = jnp.right_shift(leaf, level - 1)
        plain, flipped = coupling_forms(link_ref[level, 0])
        rank = ranks_ref[level, jnp.left_shift(child, level)]
        which = jnp.where(jnp.bitwise_and(child, 1) == 1, plain, flipped)
        joint_ref[level - 2] = jointly(which, rank, scale_of(level))
    u0 = apply_nt(pair(q_ref[:, UP:]), from0_ref[...])
    u0_ref[...] = u0
    zero = pair(u0)
    cross0 = cross0_ref[...]
    head = pair(q_ref[:, :128] - apply_nn(zero, cross0[:, :128]))
    both = packed(head, weight_ref[...])
    u1_ref[0] = both[:128]
    u1_ref[1] = both[128:]
    onward = onward_ref[...]
    for group in range(3):
        at = slice(group * 128, group * 128 + 128)
        x_ref[:, at] = q_ref[:, at] - apply_nn(zero, cross0[:, at]) - apply_nn(head, onward[:, at])


def early(ranks, coupling, q, from0, cross0, weight, onward):
    return pl.pallas_call(
        early_kernel,
        out_shape=(shape(COLS, 128), shape(2, 128, 128), shape(COLS, UP), shape(5, R, 128)),
        in_specs=[SMEM] + [VMEM] * 6,
        out_specs=(VMEM,) * 4,
        compiler_params=params(12),
        cost_estimate=cost(3e9, 4e6),
        name="early",
    )(ranks, coupling, q, from0, cross0, weight, onward)


OWN_TILE = {2: 0, 3: 3, 4: 5, 5: 7, 6: 8}
ONWARD = {2: ((1, 1), (2, 2)), 3: ((3, 1), (4, 2)), 4: ((6, 2),), 5: ((7, 2),), 6: ()}


def late_kernel(ranks_ref, joint_ref, near_ref, far_ref, x_ref, keep_ref, send_ref, pk_ref, work_ref):
    leaf, col, core = leaf_index(), lax.axis_index("cols"), lax.axis_index("core")
    for other, source in ((0, near_ref), (1, far_ref)):
        for slot, offset in enumerate((0, 1, 2, 3)):
            part = jnp.bitwise_xor(core, other) * 4 + jnp.bitwise_xor(col, offset)
            rows = pl.ds(pl.multiple_of(part * 8, 8), 8)
            for tile in range(9):
                pk_ref[tile, rows, :] = source[slot, tile]
    systems = []
    for level in range(2, 7):
        systems.append(system(joint_ref[level - 2], pk_ref[OWN_TILE[level]], level % 2 == 0))
    for item in range(5):
        work_ref[item] = systems[item]
    eliminate(work_ref, 5)
    weights, onwards = {}, {}
    for level in range(2, 7):
        child = jnp.right_shift(leaf, level - 1)
        rank = ranks_ref[level, jnp.left_shift(jnp.bitwise_xor(child, 1), level)]
        weight = solved(work_ref, level - 2, rank, scale_of(level))
        if level % 2 == 0:
            weight = pltpu.roll(weight, R, 1)
        weights[level] = weight
        onwards[level] = [(dot_high(weight, pk_ref[tile], TN), target) for tile, target in ONWARD[level]]
    groups = [x_ref[:, g * 128:g * 128 + 128] for g in range(3)]
    for level in range(2, 7):
        value = pair(groups[(level - 1) // 2])
        for onward, target in onwards[level]:
            groups[target] = groups[target] - apply_nn(value, onward)
        both = packed(value, weights[level])
        keep_ref[level - 2] = jnp.where(core == 0, both[:128], both[128:])
        send_ref[level - 2] = jnp.where(core == 0, both[128:], both[:128])


def late(ranks, joint, near, far, x):
    return pl.pallas_call(
        late_kernel,
        out_shape=(shape(5, 128, 128), shape(5, 128, 128)),
        in_specs=[SMEM] + [VMEM] * 4,
        out_specs=(VMEM,) * 2,
        scratch_shapes=[pltpu.VMEM((9, R, 128), F32), pltpu.VMEM((5, R, 128), F32)],
        compiler_params=params(16),
        cost_estimate=cost(4e9, 4e6),
        name="late",
    )(ranks, joint, near, far, x)


def turned(value):
    return pltpu.roll(value, 4, 0)


def two_kernel(keep_ref, recv_ref, two_ref):
    two_ref[...] = keep_ref[0] + recv_ref[0]


def level_two(keep, recv):
    return pl.pallas_call(
        two_kernel,
        out_shape=shape(128, 128),
        in_specs=[VMEM] * 2,
        out_specs=VMEM,
        compiler_params=params(4),
        cost_estimate=cost(1e6, 1e5),
        name="two",
    )(keep, recv)


def deal_kernel(keep_ref, recv_ref, out_ref):
    top = lax.broadcasted_iota(jnp.int32, (8, 128), 0) < 4
    for t in range(16):
        rows = slice(8 * t, 8 * t + 8)
        for group in range(2):
            first = keep_ref[2 * group + 1, rows] + recv_ref[2 * group + 1, rows]
            second = keep_ref[2 * group + 2, rows] + recv_ref[2 * group + 2, rows]
            to = slice(8 * group, 8 * group + 8)
            out_ref[2 * t, to] = jnp.where(top, first, turned(second))
            out_ref[2 * t + 1, to] = jnp.where(top, turned(first), second)


def deal(keep, recv):
    return pl.pallas_call(
        deal_kernel,
        out_shape=shape(32, 16, 128),
        in_specs=[VMEM] * 2,
        out_specs=VMEM,
        compiler_params=params(4),
        cost_estimate=cost(1e8, 1e6),
        name="deal",
    )(keep, recv)


def collect_kernel(got_ref, out_ref):
    top = lax.broadcasted_iota(jnp.int32, (8, 128), 0) < 4
    pieces = [got_ref[q] for q in range(32)]
    sums = []
    for _ in range(4):
        pieces = [pieces[2 * c] + pieces[2 * c + 1] for c in range(len(pieces) // 2)]
        sums.append(pieces)
    for e in range(32):
        parts = [sums[k][(e >> (k + 1)) ^ 1] for k in range(4)]
        out_ref[e, 0:8] = jnp.where(top, parts[0][0:8], parts[1][0:8])
        out_ref[e, 8:16] = jnp.where(top, parts[2][8:16], parts[3][8:16])


def collect(got):
    return pl.pallas_call(
        collect_kernel,
        out_shape=shape(32, 16, 128),
        in_specs=[VMEM],
        out_specs=VMEM,
        compiler_params=params(4),
        cost_estimate=cost(1e8, 1e6),
        name="collect",
    )(got)


def final_kernel(field0_ref, field1_ref, wide_ref, u0_ref, u1_ref, near2_ref, far2_ref, near_ref, far_ref,
                 out_ref, left_ref, all_ref, wide_vmem, field_vmem, sems):
    step = pl.program_id(0)
    half = step // (LEAF // BLK)
    loads = [
        pltpu.make_async_copy(
            wide_ref.at[:, j * BLK:j * BLK + BLK], wide_vmem.at[:, j * BLK:j * BLK + BLK], sems.at[j]
        )
        for j in range(8)
    ]
    loads += [
        pltpu.make_async_copy(
            field1_ref.at[:, j * BLK:j * BLK + BLK], field_vmem.at[:, j * BLK:j * BLK + BLK], sems.at[8 + j]
        )
        for j in range(4)
    ]

    @pl.when(step == 0)
    def _():
        for load in loads:
            load.start()
        core = lax.axis_index("core")
        top = lax.broadcasted_iota(jnp.int32, (8, 128), 0) < 4
        lane = lanes(8)

        def unpack(first, second, begin, group):
            columns = slice(group * 128, group * 128 + 128)
            upper = pl.ds(pl.multiple_of(begin, 8), 8)
            lower = pl.ds(pl.multiple_of(begin + 128, 8), 8)
            all_ref[upper, columns] = jnp.where(lane < R, first, pltpu.roll(second, R, 1))
            all_ref[lower, columns] = jnp.where(lane < R, pltpu.roll(first, R, 1), second)

        for two, rest, start in ((near2_ref, near_ref, core), (far2_ref, far_ref, 1 - core)):
            for t in range(16):
                rows = slice(8 * t, 8 * t + 8)
                begin = start * 256 + 8 * t
                unpack(u1_ref[start, rows], two[rows], begin, 0)
                for group in range(2):
                    one = rest[2 * t, 8 * group:8 * group + 8]
                    other = rest[2 * t + 1, 8 * group:8 * group + 8]
                    unpack(
                        jnp.where(top, one, turned(other)), jnp.where(top, turned(one), other), begin, group + 1
                    )
        high, low = split(all_ref[...])
        left_ref[:, 0:UP] = high
        left_ref[:, 512:512 + UP] = low
        high, low = split(u0_ref[...])
        left_ref[:, UP:512] = high
        left_ref[:, 512 + UP:] = low

    for j in range(8):
        @pl.when(step == j)
        def _():
            loads[j].wait()
            if j >= 4:
                loads[j + 4].wait()

    right = wide_vmem[:, pl.ds(pl.multiple_of(step * BLK, BLK), BLK)]
    update = dot(left_ref[:, :512], right, NN) + dot(left_ref[:, 512:], right, NN)

    @pl.when(half == 0)
    def _():
        out_ref[...] = field0_ref[:, pl.ds(pl.multiple_of(step * BLK, BLK), BLK)] - update

    @pl.when(half == 1)
    def _():
        out_ref[...] = field_vmem[:, pl.ds(pl.multiple_of((step - 4) * BLK, BLK), BLK)] - update


def final(field0, field1, wide, *updates):
    return pl.pallas_call(
        final_kernel,
        grid=(ROWS // BLK,),
        out_shape=shape(COLS, ROWS),
        in_specs=[
            VMEM, HBM, HBM,
        ] + [VMEM] * 6,
        out_specs=pl.BlockSpec((COLS, BLK), lambda j: (0, j)),
        scratch_shapes=[
            pltpu.VMEM((COLS, 1024), BF16), pltpu.VMEM((COLS, UP), F32), pltpu.VMEM((512, ROWS), BF16),
            pltpu.VMEM((COLS, LEAF), F32), pltpu.SemaphoreType.DMA((12,)),
        ],
        compiler_params=params(20),
        cost_estimate=cost(2 * COLS * 1024 * ROWS, 12e6),
        name="final",
    )(field0, stay(field1), stay(wide), *updates)


def swap(array, mask, axis):
    return lax.ppermute(array, axis, [(i, i ^ mask) for i in range(lax.axis_size(axis))])


def local(samples, order_perm, leaf_factor, bases, coupling, ranks):
    wide, mine, theirs, own1, gram0, cross0, samples = grams(bases, samples)
    order = order_perm.reshape(1, ROWS)
    got = swap(theirs, 1, "core")
    sib1 = swap(own1, 1, "core")
    permuted0, factor = permute_first(samples, order, leaf_factor)
    permuted1 = permute_second(samples, order)
    field0 = leaf_product(permuted0, factor, 0)
    field1 = leaf_product(permuted1, factor, 1)
    q = project(field0, field1, wide)
    from0, weight1, onward1 = solve_early(ranks, coupling, gram0, own1, sib1)
    u0, u1, x, joint = early(ranks, coupling, q, from0, cross0, weight1, onward1)

    chip = (mine + got)[3:]
    got = swap(chip, 1, "z")
    low_lane = lax.broadcasted_iota(jnp.int32, (8, 128), 1) < R
    pack = [chip[0], got[1], got[2]]
    total = chip[3:] + got[3:]
    got = swap(total, 2, "z")
    pack += [jnp.where(low_lane, total[0], got[0]), got[1]]
    total = total[2:] + got[2:]
    got = swap(total, 7, "z")
    pack += [total[0], got[1]]
    total = total[2:] + got[2:]
    got = swap(total, 1, "x")
    pack += [jnp.where(low_lane, total[0], got[0]), total[1] + got[1]]
    pack = jnp.stack(pack)
    got = swap(pack, 1, "cols")
    pack = jnp.stack([pack, got])
    got = swap(pack, 2, "cols")
    near = jnp.concatenate([pack, got], axis=0)
    far = swap(near, 1, "core")
    u1 = swap(u1, 1, "core")
    keep, send = late(ranks, joint, near, far, x)
    got = swap(send, 1, "core")
    two = level_two(keep, got)
    two = swap(two, 1, "z")
    dealt = deal(keep, got)
    got = lax.all_to_all(dealt, ("x", "z"), 0, 0, tiled=True)
    far_two = swap(two, 1, "core")
    total = collect(got)
    back = lax.all_to_all(total, ("x", "z"), 0, 0, tiled=True)
    far_back = swap(back, 1, "core")
    return final(field0, field1, wide, u0, u1, two, far_two, back, far_back)


def solution(mesh):
    fine = jax.sharding.Mesh(mesh.devices.reshape(4, 8, 2, 4), ("x", "z", "core", "cols"))
    leaf = ("x", "z", "core")
    in_specs = (
        P("cols", leaf),
        P(leaf),
        P(leaf, None, None),
        P(None, None, leaf),
        P(None, leaf, None, None),
        P(),
    )
    out_specs = P("cols", leaf)
    return jax.shard_map(local, mesh=fine, in_specs=in_specs, out_specs=out_specs, check_vma=False)
```

```python
import functools
import math

import jax
import jax.numpy as jnp
from jax import lax
from jax.experimental import pallas as pl
from jax.experimental.pallas import tpu as pltpu
from jax.sharding import PartitionSpec as P


F32, BF16 = jnp.float32, jnp.bfloat16
HIGH = lax.Precision.HIGHEST
NT = (((1,), (1,)), ((), ()))
NN = (((1,), (0,)), ((), ()))
TN = (((0,), (0,)), ((), ()))

LEAF, R, ROWS, COLS, LEVELS = 1024, 64, 2048, 512, 7
UP = (LEVELS - 1) * R
BLK = 256
MIB = 1024 * 1024
VMEM = pl.BlockSpec(memory_space=pltpu.VMEM)
SMEM = pl.BlockSpec(memory_space=pltpu.SMEM)
HBM = pl.BlockSpec(memory_space=pltpu.HBM)


def params(mib, **more):
    return pltpu.CompilerParams(vmem_limit_bytes=mib * MIB, **more)


def cost(flops, moved):
    return pl.CostEstimate(flops=int(flops), bytes_accessed=int(moved), transcendentals=0)


def shape(*dims, dtype=F32):
    return jax.ShapeDtypeStruct(dims, dtype)


def stay(array):
    return pltpu.with_memory_space_constraint(array, pltpu.HBM)


def split(value):
    high = value.astype(BF16)
    return high, (value - high.astype(F32)).astype(BF16)


def dot(left, right, dims):
    return lax.dot_general(left, right, dims, preferred_element_type=F32)


def dot_high(left, right, dims):
    return lax.dot_general(left, right, dims, precision=HIGH, preferred_element_type=F32)


def twice(value, axis):
    return jnp.concatenate([value, value], axis=axis)


def gram_kernel(bases_ref, samples_ref, wide_ref, mine_ref, theirs_ref, first_ref, gram0_ref, cross0_ref, kept_ref,
                held_ref, tiles_ref, sems):
    load = pltpu.make_async_copy(bases_ref, held_ref, sems.at[0])
    load.start()
    keep = pltpu.make_async_copy(samples_ref, kept_ref, sems.at[1])
    keep.start()
    load.wait()
    nothing = jnp.zeros((R, LEAF), BF16)
    wide_ref[0:UP] = held_ref[1:].reshape(UP, ROWS)
    wide_ref[UP:UP + R, 0:LEAF] = held_ref[0, :, 0:LEAF]
    wide_ref[UP:UP + R, LEAF:] = nothing
    wide_ref[UP + R:, 0:LEAF] = nothing
    wide_ref[UP + R:, LEAF:] = held_ref[0, :, LEAF:]
    wide = wide_ref[...]
    gram = dot(wide, wide, NT)
    first_ref[...] = gram[:R, :UP]
    tile = 0
    for level in range(6):
        for lane in range(level // 2, 3):
            for half in range(2):
                top = level * R + 32 * half
                tiles_ref[half, tile] = gram[top:top + 32, lane * 128:lane * 128 + 128]
            tile += 1
    core = lax.axis_index("core")
    mine_ref[...] = tiles_ref[core]
    theirs_ref[...] = tiles_ref[1 - core]
    gram0_ref[...] = gram[UP:, UP:]
    cross0_ref[...] = gram[UP:, :UP]
    keep.wait()


def grams(bases, samples):
    return pl.pallas_call(
        gram_kernel,
        out_shape=(
            shape(512, ROWS, dtype=BF16), shape(12, 32, 128), shape(12, 32, 128), shape(R, UP), shape(128, 128),
            shape(128, UP),
            pltpu.VMEM((COLS, ROWS), BF16),
        ),
        in_specs=[HBM] * 2,
        out_specs=(VMEM,) * 7,
        scratch_shapes=[pltpu.VMEM((LEVELS, R, ROWS), BF16), pltpu.VMEM((2, 12, 32, 128), F32), pltpu.SemaphoreType.DMA((2,))],
        compiler_params=params(14),
        cost_estimate=cost(2e9, 4e6),
        name="gram",
    )(stay(bases), stay(samples))


def permute_block(samples_ref, order_ref, out_ref, begin):
    def block(j, carry):
        columns = pl.ds(pl.multiple_of(j * BLK, BLK), BLK)
        rows = lax.broadcasted_iota(jnp.int32, (ROWS, BLK), 0)
        source = pl.ds(pl.multiple_of(begin + j * BLK, BLK), BLK)
        local = jnp.bitwise_and(order_ref[:, source], ROWS - 1)
        chosen = (rows == local).astype(F32).astype(BF16)
        out_ref[:, columns] = dot(samples_ref[...], chosen, NN).astype(BF16)
        return carry

    lax.fori_loop(0, LEAF // BLK, block, 0)


def permute_first_kernel(samples_ref, order_ref, factor_ref, out_ref, kept_ref, sem):
    keep = pltpu.make_async_copy(factor_ref, kept_ref, sem)
    keep.start()
    permute_block(samples_ref, order_ref, out_ref, 0)
    keep.wait()


def permute_second_kernel(samples_ref, order_ref, out_ref):
    permute_block(samples_ref, order_ref, out_ref, LEAF)


def permute_first(samples, order, factor):
    return pl.pallas_call(
        permute_first_kernel,
        out_shape=(shape(COLS, LEAF, dtype=BF16), pltpu.VMEM((2, LEAF, LEAF), BF16)),
        in_specs=[VMEM, VMEM, HBM],
        out_specs=(VMEM,) * 2,
        scratch_shapes=[pltpu.SemaphoreType.DMA],
        compiler_params=params(14),
        cost_estimate=cost(COLS * ROWS * ROWS, 4e6),
        name="permute_first",
    )(samples, order, stay(factor))


def permute_second(samples, order):
    return pl.pallas_call(
        permute_second_kernel,
        out_shape=shape(COLS, LEAF, dtype=BF16),
        in_specs=[VMEM, VMEM],
        out_specs=VMEM,
        compiler_params=params(10),
        cost_estimate=cost(COLS * ROWS * ROWS, 4e6),
        name="permute_second",
    )(samples, order)


def leaf_kernel(permuted_ref, factor_ref, field_ref, *, half):
    def block(j, carry):
        columns = pl.ds(pl.multiple_of(j * 512, 512), 512)
        field_ref[:, columns] = dot(permuted_ref[...], factor_ref[half, :, columns], NN)
        return carry

    lax.fori_loop(0, 2, block, 0)


def leaf_product(permuted, factor, half):
    return pl.pallas_call(
        functools.partial(leaf_kernel, half=half),
        out_shape=shape(COLS, LEAF),
        in_specs=[VMEM] * 2,
        out_specs=VMEM,
        compiler_params=params(12),
        cost_estimate=cost(2 * COLS * LEAF * LEAF, 5e6),
    )(permuted, factor)


def project_kernel(first_ref, second_ref, wide_ref, q_ref):
    def rows_of(i, carry):
        rows = pl.ds(pl.multiple_of(i * 256, 256), 256)
        total = None
        for half, source in enumerate((first_ref, second_ref)):
            for part in split(source[rows, :]):
                term = dot(part, wide_ref[:, half * LEAF:(half + 1) * LEAF], NT)
                total = term if total is None else total + term
        q_ref[rows, :] = total
        return carry

    lax.fori_loop(0, COLS // 256, rows_of, 0)


def project(first, second, wide):
    return pl.pallas_call(
        project_kernel,
        out_shape=shape(COLS, 512),
        in_specs=[VMEM] * 3,
        out_specs=VMEM,
        compiler_params=params(14),
        cost_estimate=cost(4 * COLS * 512 * ROWS, 7e6),
        name="project",
    )(first, second, wide)


def coupling_forms(link):
    flipped = link.T
    plain = twice(flipped, 0).T
    return plain, twice(link, 0).T


def lanes(rows=R):
    return lax.broadcasted_iota(jnp.int32, (rows, 128), 1)


def jointly(link_dup, rank_own, scale):
    return jnp.where(jnp.bitwise_and(lanes(), R - 1) < rank_own, link_dup * scale, 0.0)


def system(joint, gram_tile, upper_half):
    lane = lanes()
    placed = jnp.where((lane >= R) == upper_half, joint, 0.0)
    inner = dot_high(gram_tile, twice(placed, 0), NT)
    outer = dot_high(joint[:, :R], inner, NN)
    row = lax.broadcasted_iota(jnp.int32, (R, 128), 0)
    outer = outer + jnp.where(row == lane, 1.0, 0.0)
    return jnp.where(lane < R, outer, joint)


def eliminate(work_ref, count):
    row = lax.broadcasted_iota(jnp.int32, (count, R, 128), 1)
    tile_row = lax.broadcasted_iota(jnp.int32, (count, 8, 128), 1)

    def block(step, carry):
        top = pl.multiple_of(step * 8, 8)
        here = (row >= top) & (row < top + 8)
        value = work_ref[...]
        tile = work_ref[:, pl.ds(top, 8), :]
        heads = [jnp.broadcast_to(tile[:, :, j:j + 1], (count, 8, 128)) for j in range(8)]
        columns = [jnp.broadcast_to(value[:, :, j:j + 1], (count, R, 128)) for j in range(8)]
        for j in range(8):
            inverse = 1.0 / heads[j][:, j:j + 1, :]
            pivot = tile[:, j:j + 1, :] * inverse
            tile = jnp.where(tile_row == j, pivot, tile - heads[j] * pivot)
            for i in range(j + 1, 8):
                element = heads[i][:, j:j + 1, :] * inverse
                heads[i] = jnp.where(tile_row == j, element, heads[i] - heads[j] * element)
        for j in range(8):
            value = value - columns[j] * tile[:, j:j + 1, :]
        value = jnp.where(here, jnp.concatenate([tile] * 8, axis=1), value)
        work_ref[...] = pltpu.roll(value, 120, 2)
        return carry

    lax.fori_loop(0, 8, block, 0)


def solved(work_ref, item, rank_sibling, scale):
    row = lax.broadcasted_iota(jnp.int32, (R, 128), 0)
    keep = (row < rank_sibling) & (lanes() < R)
    return jnp.where(keep, work_ref[item] * scale, 0.0)


def pair(value):
    high, low = split(value)
    return jnp.concatenate([high, low], axis=1)


def apply_nt(value_pair, weight):
    high, low = split(weight)
    return dot(value_pair, twice(high, 1), NT) + dot(value_pair, twice(low, 1), NT)


def apply_nn(value_pair, weight):
    high, low = split(weight)
    return dot(value_pair, twice(high, 0), NN) + dot(value_pair, twice(low, 0), NN)


def packed(value_pair, weight):
    nothing = jnp.zeros_like(weight)
    left = jnp.concatenate([value_pair[0:128], value_pair[256:384]], axis=0)
    right = jnp.concatenate([value_pair[128:256], value_pair[384:512]], axis=0)
    return apply_nt(left, jnp.concatenate([weight, nothing], 0)) + apply_nt(right, jnp.concatenate([nothing, weight], 0))


def leaf_index():
    return (lax.axis_index("x") * 8 + lax.axis_index("z")) * 2 + lax.axis_index("core")


def scale_of(level):
    return 1.0 / math.sqrt(LEAF * 2**level)


def solve_early_kernel(ranks_ref, link_ref, gram0_ref, own1_ref, sib1_ref, from0_ref, weight_ref, onward_ref, work_ref):
    leaf = leaf_index()
    second = lax.axis_index("core")
    plain0, flipped0 = coupling_forms(link_ref[0, 0])
    plain1, flipped1 = coupling_forms(link_ref[1, 0])
    rank_f, rank_s = ranks_ref[0, 2 * leaf], ranks_ref[0, 2 * leaf + 1]
    rank_1, rank_1s = ranks_ref[1, 2 * leaf], ranks_ref[1, 2 * jnp.bitwise_xor(leaf, 1)]
    scale0, scale1 = scale_of(0), scale_of(1)
    work_ref[0] = system(jointly(flipped0, rank_f, scale0), gram0_ref[0:R], False)
    work_ref[1] = system(jointly(plain0, rank_s, scale0), gram0_ref[R:], True)
    joint1 = jointly(jnp.where(second == 1, plain1, flipped1), rank_1, scale1)
    work_ref[2] = system(joint1, own1_ref[:, :128], False)
    eliminate(work_ref, 3)
    from0_ref[R:] = solved(work_ref, 0, rank_s, scale0)
    from0_ref[0:R] = pltpu.roll(solved(work_ref, 1, rank_f, scale0), R, 1)
    weight = solved(work_ref, 2, rank_1s, scale1)
    weight_ref[...] = weight
    onward_ref[...] = dot_high(weight, sib1_ref[...], TN)


def solve_early(ranks, coupling, gram0, own1, sib1):
    return pl.pallas_call(
        solve_early_kernel,
        out_shape=(shape(128, 128), shape(R, 128), shape(128, UP)),
        in_specs=[SMEM] + [VMEM] * 4,
        out_specs=(VMEM,) * 3,
        scratch_shapes=[pltpu.VMEM((3, R, 128), F32)],
        compiler_params=params(8),
        cost_estimate=cost(3e9, 4e6),
        name="solve_early",
    )(ranks, coupling, gram0, own1, sib1)


def early_kernel(ranks_ref, link_ref, q_ref, from0_ref, cross0_ref, weight_ref, onward_ref,
                 u0_ref, u1_ref, x_ref, joint_ref):
    leaf = leaf_index()
    for level in range(2, 7):
        child = jnp.right_shift(leaf, level - 1)
        plain, flipped = coupling_forms(link_ref[level, 0])
        rank = ranks_ref[level, jnp.left_shift(child, level)]
        which = jnp.where(jnp.bitwise_and(child, 1) == 1, plain, flipped)
        joint_ref[level - 2] = jointly(which, rank, scale_of(level))
    u0 = apply_nt(pair(q_ref[:, UP:]), from0_ref[...])
    u0_ref[...] = u0
    zero = pair(u0)
    cross0 = cross0_ref[...]
    head = pair(q_ref[:, :128] - apply_nn(zero, cross0[:, :128]))
    both = packed(head, weight_ref[...])
    u1_ref[0] = both[:128]
    u1_ref[1] = both[128:]
    onward = onward_ref[...]
    for group in range(3):
        at = slice(group * 128, group * 128 + 128)
        x_ref[:, at] = q_ref[:, at] - apply_nn(zero, cross0[:, at]) - apply_nn(head, onward[:, at])


def early(ranks, coupling, q, from0, cross0, weight, onward):
    return pl.pallas_call(
        early_kernel,
        out_shape=(shape(COLS, 128), shape(2, 128, 128), shape(COLS, UP), shape(5, R, 128)),
        in_specs=[SMEM] + [VMEM] * 6,
        out_specs=(VMEM,) * 4,
        compiler_params=params(12),
        cost_estimate=cost(3e9, 4e6),
        name="early",
    )(ranks, coupling, q, from0, cross0, weight, onward)


OWN_TILE = {2: 0, 3: 3, 4: 5, 5: 7, 6: 8}
ONWARD = {2: ((1, 1), (2, 2)), 3: ((3, 1), (4, 2)), 4: ((6, 2),), 5: ((7, 2),), 6: ()}


def late_kernel(ranks_ref, joint_ref, near_ref, far_ref, x_ref, keep_ref, send_ref, pk_ref, work_ref):
    leaf, core = leaf_index(), lax.axis_index("core")
    for other, source in ((0, near_ref), (1, far_ref)):
        rows = pl.ds(pl.multiple_of(jnp.bitwise_xor(core, other) * 32, 32), 32)
        for tile in range(9):
            pk_ref[tile, rows, :] = source[tile]
    systems = []
    for level in range(2, 7):
        systems.append(system(joint_ref[level - 2], pk_ref[OWN_TILE[level]], level % 2 == 0))
    for item in range(5):
        work_ref[item] = systems[item]
    eliminate(work_ref, 5)
    weights, onwards = {}, {}
    for level in range(2, 7):
        child = jnp.right_shift(leaf, level - 1)
        rank = ranks_ref[level, jnp.left_shift(jnp.bitwise_xor(child, 1), level)]
        weight = solved(work_ref, level - 2, rank, scale_of(level))
        if level % 2 == 0:
            weight = pltpu.roll(weight, R, 1)
        weights[level] = weight
        onwards[level] = [(dot_high(weight, pk_ref[tile], TN), target) for tile, target in ONWARD[level]]
    groups = [x_ref[:, g * 128:g * 128 + 128] for g in range(3)]
    for level in range(2, 7):
        value = pair(groups[(level - 1) // 2])
        for onward, target in onwards[level]:
            groups[target] = groups[target] - apply_nn(value, onward)
        both = packed(value, weights[level])
        keep_ref[level - 2] = jnp.where(core == 0, both[:128], both[128:])
        send_ref[level - 2] = jnp.where(core == 0, both[128:], both[:128])


def late(ranks, joint, near, far, x):
    return pl.pallas_call(
        late_kernel,
        out_shape=(shape(5, 128, 128), shape(5, 128, 128)),
        in_specs=[SMEM] + [VMEM] * 4,
        out_specs=(VMEM,) * 2,
        scratch_shapes=[pltpu.VMEM((9, R, 128), F32), pltpu.VMEM((5, R, 128), F32)],
        compiler_params=params(16),
        cost_estimate=cost(4e9, 4e6),
        name="late",
    )(ranks, joint, near, far, x)


def turned(value):
    return pltpu.roll(value, 4, 0)


def two_kernel(keep_ref, recv_ref, two_ref):
    two_ref[...] = keep_ref[0] + recv_ref[0]


def level_two(keep, recv):
    return pl.pallas_call(
        two_kernel,
        out_shape=shape(128, 128),
        in_specs=[VMEM] * 2,
        out_specs=VMEM,
        compiler_params=params(4),
        cost_estimate=cost(1e6, 1e5),
        name="two",
    )(keep, recv)


def deal_kernel(keep_ref, recv_ref, out_ref):
    top = lax.broadcasted_iota(jnp.int32, (8, 128), 0) < 4
    for t in range(16):
        rows = slice(8 * t, 8 * t + 8)
        for group in range(2):
            first = keep_ref[2 * group + 1, rows] + recv_ref[2 * group + 1, rows]
            second = keep_ref[2 * group + 2, rows] + recv_ref[2 * group + 2, rows]
            to = slice(8 * group, 8 * group + 8)
            out_ref[2 * t, to] = jnp.where(top, first, turned(second))
            out_ref[2 * t + 1, to] = jnp.where(top, turned(first), second)


def deal(keep, recv):
    return pl.pallas_call(
        deal_kernel,
        out_shape=shape(32, 16, 128),
        in_specs=[VMEM] * 2,
        out_specs=VMEM,
        compiler_params=params(4),
        cost_estimate=cost(1e8, 1e6),
        name="deal",
    )(keep, recv)


def collect_kernel(got_ref, out_ref):
    top = lax.broadcasted_iota(jnp.int32, (8, 128), 0) < 4
    pieces = [got_ref[q] for q in range(32)]
    sums = []
    for _ in range(4):
        pieces = [pieces[2 * c] + pieces[2 * c + 1] for c in range(len(pieces) // 2)]
        sums.append(pieces)
    for e in range(32):
        parts = [sums[k][(e >> (k + 1)) ^ 1] for k in range(4)]
        out_ref[e, 0:8] = jnp.where(top, parts[0][0:8], parts[1][0:8])
        out_ref[e, 8:16] = jnp.where(top, parts[2][8:16], parts[3][8:16])


def collect(got):
    return pl.pallas_call(
        collect_kernel,
        out_shape=shape(32, 16, 128),
        in_specs=[VMEM],
        out_specs=VMEM,
        compiler_params=params(4),
        cost_estimate=cost(1e8, 1e6),
        name="collect",
    )(got)


def final_kernel(field0_ref, field1_ref, wide_ref, u0_ref, u1_ref, near2_ref, far2_ref, near_ref, far_ref,
                 out_ref, left_ref, all_ref, wide_vmem, field_vmem, sems):
    step = pl.program_id(0)
    half = step // (LEAF // BLK)
    loads = [
        pltpu.make_async_copy(
            wide_ref.at[:, j * BLK:j * BLK + BLK], wide_vmem.at[:, j * BLK:j * BLK + BLK], sems.at[j]
        )
        for j in range(8)
    ]
    loads += [
        pltpu.make_async_copy(
            field1_ref.at[:, j * BLK:j * BLK + BLK], field_vmem.at[:, j * BLK:j * BLK + BLK], sems.at[8 + j]
        )
        for j in range(4)
    ]

    @pl.when(step == 0)
    def _():
        for load in loads:
            load.start()
        core = lax.axis_index("core")
        top = lax.broadcasted_iota(jnp.int32, (8, 128), 0) < 4
        lane = lanes(8)

        def unpack(first, second, begin, group):
            columns = slice(group * 128, group * 128 + 128)
            upper = pl.ds(pl.multiple_of(begin, 8), 8)
            lower = pl.ds(pl.multiple_of(begin + 128, 8), 8)
            all_ref[upper, columns] = jnp.where(lane < R, first, pltpu.roll(second, R, 1))
            all_ref[lower, columns] = jnp.where(lane < R, pltpu.roll(first, R, 1), second)

        for two, rest, start in ((near2_ref, near_ref, core), (far2_ref, far_ref, 1 - core)):
            for t in range(16):
                rows = slice(8 * t, 8 * t + 8)
                begin = start * 256 + 8 * t
                unpack(u1_ref[start, rows], two[rows], begin, 0)
                for group in range(2):
                    one = rest[2 * t, 8 * group:8 * group + 8]
                    other = rest[2 * t + 1, 8 * group:8 * group + 8]
                    unpack(
                        jnp.where(top, one, turned(other)), jnp.where(top, turned(one), other), begin, group + 1
                    )
        high, low = split(all_ref[...])
        left_ref[:, 0:UP] = high
        left_ref[:, 512:512 + UP] = low
        high, low = split(u0_ref[...])
        left_ref[:, UP:512] = high
        left_ref[:, 512 + UP:] = low

    for j in range(8):
        @pl.when(step == j)
        def _():
            loads[j].wait()
            if j >= 4:
                loads[j + 4].wait()

    right = wide_vmem[:, pl.ds(pl.multiple_of(step * BLK, BLK), BLK)]
    update = dot(left_ref[:, :512], right, NN) + dot(left_ref[:, 512:], right, NN)

    @pl.when(half == 0)
    def _():
        out_ref[...] = field0_ref[:, pl.ds(pl.multiple_of(step * BLK, BLK), BLK)] - update

    @pl.when(half == 1)
    def _():
        out_ref[...] = field_vmem[:, pl.ds(pl.multiple_of((step - 4) * BLK, BLK), BLK)] - update


def final(field0, field1, wide, *updates):
    return pl.pallas_call(
        final_kernel,
        grid=(ROWS // BLK,),
        out_shape=shape(COLS, ROWS),
        in_specs=[
            VMEM, HBM, HBM,
        ] + [VMEM] * 6,
        out_specs=pl.BlockSpec((COLS, BLK), lambda j: (0, j)),
        scratch_shapes=[
            pltpu.VMEM((COLS, 1024), BF16), pltpu.VMEM((COLS, UP), F32), pltpu.VMEM((512, ROWS), BF16),
            pltpu.VMEM((COLS, LEAF), F32), pltpu.SemaphoreType.DMA((12,)),
        ],
        compiler_params=params(20),
        cost_estimate=cost(2 * COLS * 1024 * ROWS, 12e6),
        name="final",
    )(field0, stay(field1), stay(wide), *updates)


def swap(array, mask, axis):
    return lax.ppermute(array, axis, [(i, i ^ mask) for i in range(lax.axis_size(axis))])


def local(samples, order_perm, leaf_factor, bases, coupling, ranks):
    wide, mine, theirs, own1, gram0, cross0, samples = grams(bases, samples)
    order = order_perm.reshape(1, ROWS)
    got = swap(theirs, 1, "core")
    sib1 = swap(own1, 1, "core")
    permuted0, factor = permute_first(samples, order, leaf_factor)
    permuted1 = permute_second(samples, order)
    field0 = leaf_product(permuted0, factor, 0)
    field1 = leaf_product(permuted1, factor, 1)
    q = project(field0, field1, wide)
    from0, weight1, onward1 = solve_early(ranks, coupling, gram0, own1, sib1)
    u0, u1, x, joint = early(ranks, coupling, q, from0, cross0, weight1, onward1)

    chip = (mine + got)[3:]
    got = swap(chip, 1, "z")
    low_lane = lax.broadcasted_iota(jnp.int32, (32, 128), 1) < R
    pack = [chip[0], got[1], got[2]]
    total = chip[3:] + got[3:]
    got = swap(total, 2, "z")
    pack += [jnp.where(low_lane, total[0], got[0]), got[1]]
    total = total[2:] + got[2:]
    got = swap(total, 7, "z")
    pack += [total[0], got[1]]
    total = total[2:] + got[2:]
    got = swap(total, 1, "x")
    pack += [jnp.where(low_lane, total[0], got[0]), total[1] + got[1]]
    near = jnp.stack(pack)
    far = swap(near, 1, "core")
    u1 = swap(u1, 1, "core")
    keep, send = late(ranks, joint, near, far, x)
    got = swap(send, 1, "core")
    two = level_two(keep, got)
    two = swap(two, 1, "z")
    dealt = deal(keep, got)
    got = lax.all_to_all(dealt, ("x", "z"), 0, 0, tiled=True)
    far_two = swap(two, 1, "core")
    total = collect(got)
    back = lax.all_to_all(total, ("x", "z"), 0, 0, tiled=True)
    far_back = swap(back, 1, "core")
    return final(field0, field1, wide, u0, u1, two, far_two, back, far_back)


def solution(mesh):
    fine = jax.sharding.Mesh(mesh.devices.reshape(4, 8, 2, 4), ("x", "z", "core", "cols"))
    leaf = ("x", "z", "core")
    in_specs = (
        P("cols", leaf),
        P(leaf),
        P(leaf, None, None),
        P(None, None, leaf),
        P(None, leaf, None, None),
        P(),
    )
    out_specs = P("cols", leaf)
    return jax.shard_map(local, mesh=fine, in_specs=in_specs, out_specs=out_specs, check_vma=False)
```

```python
import functools
import math

import jax
import jax.numpy as jnp
from jax import lax
from jax.experimental import pallas as pl
from jax.experimental.pallas import tpu as pltpu
from jax.sharding import PartitionSpec as P


F32, BF16 = jnp.float32, jnp.bfloat16
HIGH = lax.Precision.HIGHEST
NT = (((1,), (1,)), ((), ()))
NN = (((1,), (0,)), ((), ()))
TN = (((0,), (0,)), ((), ()))

LEAF, R, ROWS, COLS, LEVELS = 1024, 64, 2048, 512, 7
UP = (LEVELS - 1) * R
BLK = 256
MIB = 1024 * 1024
VMEM = pl.BlockSpec(memory_space=pltpu.VMEM)
SMEM = pl.BlockSpec(memory_space=pltpu.SMEM)
HBM = pl.BlockSpec(memory_space=pltpu.HBM)


def params(mib, **more):
    return pltpu.CompilerParams(vmem_limit_bytes=mib * MIB, **more)


def cost(flops, moved):
    return pl.CostEstimate(flops=int(flops), bytes_accessed=int(moved), transcendentals=0)


def shape(*dims, dtype=F32):
    return jax.ShapeDtypeStruct(dims, dtype)


def stay(array):
    return pltpu.with_memory_space_constraint(array, pltpu.HBM)


def split(value):
    high = value.astype(BF16)
    return high, (value - high.astype(F32)).astype(BF16)


def dot(left, right, dims):
    return lax.dot_general(left, right, dims, preferred_element_type=F32)


def dot_high(left, right, dims):
    return lax.dot_general(left, right, dims, precision=HIGH, preferred_element_type=F32)


def twice(value, axis):
    return jnp.concatenate([value, value], axis=axis)


def gram_kernel(bases_ref, samples_ref, wide_ref, mine_ref, theirs_ref, first_ref, gram0_ref, cross0_ref, kept_ref,
                held_ref, tiles_ref, sems):
    load = pltpu.make_async_copy(bases_ref, held_ref, sems.at[0])
    load.start()
    keep = pltpu.make_async_copy(samples_ref, kept_ref, sems.at[1])
    keep.start()
    load.wait()
    nothing = jnp.zeros((R, LEAF), BF16)
    wide_ref[0:UP] = held_ref[1:].reshape(UP, ROWS)
    wide_ref[UP:UP + R, 0:LEAF] = held_ref[0, :, 0:LEAF]
    wide_ref[UP:UP + R, LEAF:] = nothing
    wide_ref[UP + R:, 0:LEAF] = nothing
    wide_ref[UP + R:, LEAF:] = held_ref[0, :, LEAF:]
    wide = wide_ref[...]
    gram = dot(wide, wide, NT)
    first_ref[...] = gram[:R, :UP]
    tile = 0
    for level in range(6):
        for lane in range(level // 2, 3):
            for half in range(2):
                top = level * R + 32 * half
                tiles_ref[half, tile] = gram[top:top + 32, lane * 128:lane * 128 + 128]
            tile += 1
    core = lax.axis_index("core")
    mine_ref[...] = tiles_ref[core]
    theirs_ref[...] = tiles_ref[1 - core]
    gram0_ref[...] = gram[UP:, UP:]
    cross0_ref[...] = gram[UP:, :UP]
    keep.wait()


def grams(bases, samples):
    return pl.pallas_call(
        gram_kernel,
        out_shape=(
            shape(512, ROWS, dtype=BF16), shape(12, 32, 128), shape(12, 32, 128), shape(R, UP), shape(128, 128),
            shape(128, UP),
            pltpu.VMEM((COLS, ROWS), BF16),
        ),
        in_specs=[HBM] * 2,
        out_specs=(VMEM,) * 7,
        scratch_shapes=[pltpu.VMEM((LEVELS, R, ROWS), BF16), pltpu.VMEM((2, 12, 32, 128), F32), pltpu.SemaphoreType.DMA((2,))],
        compiler_params=params(14),
        cost_estimate=cost(2e9, 4e6),
        name="gram",
    )(stay(bases), stay(samples))


def permute_block(samples_ref, order_ref, out_ref, begin):
    def block(j, carry):
        columns = pl.ds(pl.multiple_of(j * BLK, BLK), BLK)
        rows = lax.broadcasted_iota(jnp.int32, (ROWS, BLK), 0)
        source = pl.ds(pl.multiple_of(begin + j * BLK, BLK), BLK)
        local = jnp.bitwise_and(order_ref[:, source], ROWS - 1)
        chosen = (rows == local).astype(F32).astype(BF16)
        out_ref[:, columns] = dot(samples_ref[...], chosen, NN).astype(BF16)
        return carry

    lax.fori_loop(0, LEAF // BLK, block, 0)


def permute_first_kernel(samples_ref, order_ref, factor_ref, out_ref, kept_ref, sem):
    keep = pltpu.make_async_copy(factor_ref, kept_ref, sem)
    keep.start()
    permute_block(samples_ref, order_ref, out_ref, 0)
    keep.wait()


def permute_second_kernel(samples_ref, order_ref, out_ref):
    permute_block(samples_ref, order_ref, out_ref, LEAF)


def permute_first(samples, order, factor):
    return pl.pallas_call(
        permute_first_kernel,
        out_shape=(shape(COLS, LEAF, dtype=BF16), pltpu.VMEM((2, LEAF, LEAF), BF16)),
        in_specs=[VMEM, VMEM, HBM],
        out_specs=(VMEM,) * 2,
        scratch_shapes=[pltpu.SemaphoreType.DMA],
        compiler_params=params(14),
        cost_estimate=cost(COLS * ROWS * ROWS, 4e6),
        name="permute_first",
    )(samples, order, stay(factor))


def permute_second(samples, order):
    return pl.pallas_call(
        permute_second_kernel,
        out_shape=shape(COLS, LEAF, dtype=BF16),
        in_specs=[VMEM, VMEM],
        out_specs=VMEM,
        compiler_params=params(10),
        cost_estimate=cost(COLS * ROWS * ROWS, 4e6),
        name="permute_second",
    )(samples, order)


def leaf_kernel(permuted_ref, factor_ref, field_ref, *, half):
    def block(j, carry):
        columns = pl.ds(pl.multiple_of(j * 512, 512), 512)
        field_ref[:, columns] = dot(permuted_ref[...], factor_ref[half, :, columns], NN)
        return carry

    lax.fori_loop(0, 2, block, 0)


def leaf_product(permuted, factor, half):
    return pl.pallas_call(
        functools.partial(leaf_kernel, half=half),
        out_shape=shape(COLS, LEAF),
        in_specs=[VMEM] * 2,
        out_specs=VMEM,
        compiler_params=params(12),
        cost_estimate=cost(2 * COLS * LEAF * LEAF, 5e6),
    )(permuted, factor)


def project_kernel(first_ref, second_ref, wide_ref, q_ref):
    def rows_of(i, carry):
        rows = pl.ds(pl.multiple_of(i * 256, 256), 256)
        total = None
        for half, source in enumerate((first_ref, second_ref)):
            for part in split(source[rows, :]):
                term = dot(part, wide_ref[:, half * LEAF:(half + 1) * LEAF], NT)
                total = term if total is None else total + term
        q_ref[rows, :] = total
        return carry

    lax.fori_loop(0, COLS // 256, rows_of, 0)


def project(first, second, wide):
    return pl.pallas_call(
        project_kernel,
        out_shape=shape(COLS, 512),
        in_specs=[VMEM] * 3,
        out_specs=VMEM,
        compiler_params=params(14),
        cost_estimate=cost(4 * COLS * 512 * ROWS, 7e6),
        name="project",
    )(first, second, wide)


def coupling_forms(link):
    flipped = link.T
    plain = twice(flipped, 0).T
    return plain, twice(link, 0).T


def lanes(rows=R):
    return lax.broadcasted_iota(jnp.int32, (rows, 128), 1)


def jointly(link_dup, rank_own, scale):
    return jnp.where(jnp.bitwise_and(lanes(), R - 1) < rank_own, link_dup * scale, 0.0)


def system(joint, gram_tile, upper_half):
    lane = lanes()
    placed = jnp.where((lane >= R) == upper_half, joint, 0.0)
    inner = dot_high(gram_tile, twice(placed, 0), NT)
    outer = dot_high(joint[:, :R], inner, NN)
    row = lax.broadcasted_iota(jnp.int32, (R, 128), 0)
    outer = outer + jnp.where(row == lane, 1.0, 0.0)
    return jnp.where(lane < R, outer, joint)


def eliminate(work_ref, count):
    row = lax.broadcasted_iota(jnp.int32, (count, R, 128), 1)
    tile_row = lax.broadcasted_iota(jnp.int32, (count, 8, 128), 1)
    value = work_ref[...]
    for top in range(0, R, 8):
        here = (row >= top) & (row < top + 8)
        tile = value[:, top:top + 8, :]
        heads = [jnp.broadcast_to(tile[:, :, j:j + 1], (count, 8, 128)) for j in range(top, top + 8)]
        columns = [jnp.broadcast_to(value[:, :, j:j + 1], (count, R, 128)) for j in range(top, top + 8)]
        for j in range(8):
            inverse = 1.0 / heads[j][:, j:j + 1, :]
            pivot = tile[:, j:j + 1, :] * inverse
            tile = jnp.where(tile_row == j, pivot, tile - heads[j] * pivot)
            for i in range(j + 1, 8):
                element = heads[i][:, j:j + 1, :] * inverse
                heads[i] = jnp.where(tile_row == j, element, heads[i] - heads[j] * element)
        for j in range(8):
            value = value - columns[j] * tile[:, j:j + 1, :]
        value = jnp.where(here, jnp.concatenate([tile] * 8, axis=1), value)
    work_ref[...] = pltpu.roll(value, R, 2)


def solved(work_ref, item, rank_sibling, scale):
    row = lax.broadcasted_iota(jnp.int32, (R, 128), 0)
    keep = (row < rank_sibling) & (lanes() < R)
    return jnp.where(keep, work_ref[item] * scale, 0.0)


def pair(value):
    high, low = split(value)
    return jnp.concatenate([high, low], axis=1)


def apply_nt(value_pair, weight):
    high, low = split(weight)
    return dot(value_pair, twice(high, 1), NT) + dot(value_pair, twice(low, 1), NT)


def apply_nn(value_pair, weight):
    high, low = split(weight)
    return dot(value_pair, twice(high, 0), NN) + dot(value_pair, twice(low, 0), NN)


def packed(value_pair, weight):
    nothing = jnp.zeros_like(weight)
    left = jnp.concatenate([value_pair[0:128], value_pair[256:384]], axis=0)
    right = jnp.concatenate([value_pair[128:256], value_pair[384:512]], axis=0)
    return apply_nt(left, jnp.concatenate([weight, nothing], 0)) + apply_nt(right, jnp.concatenate([nothing, weight], 0))


def leaf_index():
    return (lax.axis_index("x") * 8 + lax.axis_index("z")) * 2 + lax.axis_index("core")


def scale_of(level):
    return 1.0 / math.sqrt(LEAF * 2**level)


def solve_early_kernel(ranks_ref, link_ref, gram0_ref, own1_ref, sib1_ref, from0_ref, weight_ref, onward_ref, work_ref):
    leaf = leaf_index()
    second = lax.axis_index("core")
    plain0, flipped0 = coupling_forms(link_ref[0, 0])
    plain1, flipped1 = coupling_forms(link_ref[1, 0])
    rank_f, rank_s = ranks_ref[0, 2 * leaf], ranks_ref[0, 2 * leaf + 1]
    rank_1, rank_1s = ranks_ref[1, 2 * leaf], ranks_ref[1, 2 * jnp.bitwise_xor(leaf, 1)]
    scale0, scale1 = scale_of(0), scale_of(1)
    work_ref[0] = system(jointly(flipped0, rank_f, scale0), gram0_ref[0:R], False)
    work_ref[1] = system(jointly(plain0, rank_s, scale0), gram0_ref[R:], True)
    joint1 = jointly(jnp.where(second == 1, plain1, flipped1), rank_1, scale1)
    work_ref[2] = system(joint1, own1_ref[:, :128], False)
    eliminate(work_ref, 3)
    from0_ref[R:] = solved(work_ref, 0, rank_s, scale0)
    from0_ref[0:R] = pltpu.roll(solved(work_ref, 1, rank_f, scale0), R, 1)
    weight = solved(work_ref, 2, rank_1s, scale1)
    weight_ref[...] = weight
    onward_ref[...] = dot_high(weight, sib1_ref[...], TN)


def solve_early(ranks, coupling, gram0, own1, sib1):
    return pl.pallas_call(
        solve_early_kernel,
        out_shape=(shape(128, 128), shape(R, 128), shape(128, UP)),
        in_specs=[SMEM] + [VMEM] * 4,
        out_specs=(VMEM,) * 3,
        scratch_shapes=[pltpu.VMEM((3, R, 128), F32)],
        compiler_params=params(8),
        cost_estimate=cost(3e9, 4e6),
        name="solve_early",
    )(ranks, coupling, gram0, own1, sib1)


def early_kernel(ranks_ref, link_ref, q_ref, from0_ref, cross0_ref, weight_ref, onward_ref,
                 u0_ref, u1_ref, x_ref, joint_ref):
    leaf = leaf_index()
    for level in range(2, 7):
        child = jnp.right_shift(leaf, level - 1)
        plain, flipped = coupling_forms(link_ref[level, 0])
        rank = ranks_ref[level, jnp.left_shift(child, level)]
        which = jnp.where(jnp.bitwise_and(child, 1) == 1, plain, flipped)
        joint_ref[level - 2] = jointly(which, rank, scale_of(level))
    u0 = apply_nt(pair(q_ref[:, UP:]), from0_ref[...])
    u0_ref[...] = u0
    zero = pair(u0)
    cross0 = cross0_ref[...]
    head = pair(q_ref[:, :128] - apply_nn(zero, cross0[:, :128]))
    both = packed(head, weight_ref[...])
    u1_ref[0] = both[:128]
    u1_ref[1] = both[128:]
    onward = onward_ref[...]
    for group in range(3):
        at = slice(group * 128, group * 128 + 128)
        x_ref[:, at] = q_ref[:, at] - apply_nn(zero, cross0[:, at]) - apply_nn(head, onward[:, at])


def early(ranks, coupling, q, from0, cross0, weight, onward):
    return pl.pallas_call(
        early_kernel,
        out_shape=(shape(COLS, 128), shape(2, 128, 128), shape(COLS, UP), shape(5, R, 128)),
        in_specs=[SMEM] + [VMEM] * 6,
        out_specs=(VMEM,) * 4,
        compiler_params=params(12),
        cost_estimate=cost(3e9, 4e6),
        name="early",
    )(ranks, coupling, q, from0, cross0, weight, onward)


OWN_TILE = {2: 0, 3: 3, 4: 5, 5: 7, 6: 8}
ONWARD = {2: ((1, 1), (2, 2)), 3: ((3, 1), (4, 2)), 4: ((6, 2),), 5: ((7, 2),), 6: ()}


def late_kernel(ranks_ref, joint_ref, near_ref, far_ref, x_ref, keep_ref, send_ref, pk_ref, work_ref):
    leaf, core = leaf_index(), lax.axis_index("core")
    for other, source in ((0, near_ref), (1, far_ref)):
        rows = pl.ds(pl.multiple_of(jnp.bitwise_xor(core, other) * 32, 32), 32)
        for tile in range(9):
            pk_ref[tile, rows, :] = source[tile]
    systems = []
    for level in range(2, 7):
        systems.append(system(joint_ref[level - 2], pk_ref[OWN_TILE[level]], level % 2 == 0))
    for item in range(5):
        work_ref[item] = systems[item]
    eliminate(work_ref, 5)
    weights, onwards = {}, {}
    for level in range(2, 7):
        child = jnp.right_shift(leaf, level - 1)
        rank = ranks_ref[level, jnp.left_shift(jnp.bitwise_xor(child, 1), level)]
        weight = solved(work_ref, level - 2, rank, scale_of(level))
        if level % 2 == 0:
            weight = pltpu.roll(weight, R, 1)
        weights[level] = weight
        onwards[level] = [(dot_high(weight, pk_ref[tile], TN), target) for tile, target in ONWARD[level]]
    groups = [x_ref[:, g * 128:g * 128 + 128] for g in range(3)]
    for level in range(2, 7):
        value = pair(groups[(level - 1) // 2])
        for onward, target in onwards[level]:
            groups[target] = groups[target] - apply_nn(value, onward)
        both = packed(value, weights[level])
        keep_ref[level - 2] = jnp.where(core == 0, both[:128], both[128:])
        send_ref[level - 2] = jnp.where(core == 0, both[128:], both[:128])


def late(ranks, joint, near, far, x):
    return pl.pallas_call(
        late_kernel,
        out_shape=(shape(5, 128, 128), shape(5, 128, 128)),
        in_specs=[SMEM] + [VMEM] * 4,
        out_specs=(VMEM,) * 2,
        scratch_shapes=[pltpu.VMEM((9, R, 128), F32), pltpu.VMEM((5, R, 128), F32)],
        compiler_params=params(16),
        cost_estimate=cost(4e9, 4e6),
        name="late",
    )(ranks, joint, near, far, x)


def turned(value):
    return pltpu.roll(value, 4, 0)


def two_kernel(keep_ref, recv_ref, two_ref):
    two_ref[...] = keep_ref[0] + recv_ref[0]


def level_two(keep, recv):
    return pl.pallas_call(
        two_kernel,
        out_shape=shape(128, 128),
        in_specs=[VMEM] * 2,
        out_specs=VMEM,
        compiler_params=params(4),
        cost_estimate=cost(1e6, 1e5),
        name="two",
    )(keep, recv)


def deal_kernel(keep_ref, recv_ref, out_ref):
    top = lax.broadcasted_iota(jnp.int32, (8, 128), 0) < 4
    for t in range(16):
        rows = slice(8 * t, 8 * t + 8)
        for group in range(2):
            first = keep_ref[2 * group + 1, rows] + recv_ref[2 * group + 1, rows]
            second = keep_ref[2 * group + 2, rows] + recv_ref[2 * group + 2, rows]
            to = slice(8 * group, 8 * group + 8)
            out_ref[2 * t, to] = jnp.where(top, first, turned(second))
            out_ref[2 * t + 1, to] = jnp.where(top, turned(first), second)


def deal(keep, recv):
    return pl.pallas_call(
        deal_kernel,
        out_shape=shape(32, 16, 128),
        in_specs=[VMEM] * 2,
        out_specs=VMEM,
        compiler_params=params(4),
        cost_estimate=cost(1e8, 1e6),
        name="deal",
    )(keep, recv)


def collect_kernel(got_ref, out_ref):
    top = lax.broadcasted_iota(jnp.int32, (8, 128), 0) < 4
    pieces = [got_ref[q] for q in range(32)]
    sums = []
    for _ in range(4):
        pieces = [pieces[2 * c] + pieces[2 * c + 1] for c in range(len(pieces) // 2)]
        sums.append(pieces)
    for e in range(32):
        parts = [sums[k][(e >> (k + 1)) ^ 1] for k in range(4)]
        out_ref[e, 0:8] = jnp.where(top, parts[0][0:8], parts[1][0:8])
        out_ref[e, 8:16] = jnp.where(top, parts[2][8:16], parts[3][8:16])


def collect(got):
    return pl.pallas_call(
        collect_kernel,
        out_shape=shape(32, 16, 128),
        in_specs=[VMEM],
        out_specs=VMEM,
        compiler_params=params(4),
        cost_estimate=cost(1e8, 1e6),
        name="collect",
    )(got)


def final_kernel(field0_ref, field1_ref, wide_ref, u0_ref, u1_ref, near2_ref, far2_ref, near_ref, far_ref,
                 out_ref, left_ref, all_ref, wide_vmem, field_vmem, sems):
    step = pl.program_id(0)
    half = step // (LEAF // BLK)
    loads = [
        pltpu.make_async_copy(
            wide_ref.at[:, j * BLK:j * BLK + BLK], wide_vmem.at[:, j * BLK:j * BLK + BLK], sems.at[j]
        )
        for j in range(8)
    ]
    loads += [
        pltpu.make_async_copy(
            field1_ref.at[:, j * BLK:j * BLK + BLK], field_vmem.at[:, j * BLK:j * BLK + BLK], sems.at[8 + j]
        )
        for j in range(4)
    ]

    @pl.when(step == 0)
    def _():
        for load in loads:
            load.start()
        core = lax.axis_index("core")
        top = lax.broadcasted_iota(jnp.int32, (8, 128), 0) < 4
        lane = lanes(8)

        def unpack(first, second, begin, group):
            columns = slice(group * 128, group * 128 + 128)
            upper = pl.ds(pl.multiple_of(begin, 8), 8)
            lower = pl.ds(pl.multiple_of(begin + 128, 8), 8)
            all_ref[upper, columns] = jnp.where(lane < R, first, pltpu.roll(second, R, 1))
            all_ref[lower, columns] = jnp.where(lane < R, pltpu.roll(first, R, 1), second)

        for two, rest, start in ((near2_ref, near_ref, core), (far2_ref, far_ref, 1 - core)):
            for t in range(16):
                rows = slice(8 * t, 8 * t + 8)
                begin = start * 256 + 8 * t
                unpack(u1_ref[start, rows], two[rows], begin, 0)
                for group in range(2):
                    one = rest[2 * t, 8 * group:8 * group + 8]
                    other = rest[2 * t + 1, 8 * group:8 * group + 8]
                    unpack(
                        jnp.where(top, one, turned(other)), jnp.where(top, turned(one), other), begin, group + 1
                    )
        high, low = split(all_ref[...])
        left_ref[:, 0:UP] = high
        left_ref[:, 512:512 + UP] = low
        high, low = split(u0_ref[...])
        left_ref[:, UP:512] = high
        left_ref[:, 512 + UP:] = low

    for j in range(8):
        @pl.when(step == j)
        def _():
            loads[j].wait()
            if j >= 4:
                loads[j + 4].wait()

    right = wide_vmem[:, pl.ds(pl.multiple_of(step * BLK, BLK), BLK)]
    update = dot(left_ref[:, :512], right, NN) + dot(left_ref[:, 512:], right, NN)

    @pl.when(half == 0)
    def _():
        out_ref[...] = field0_ref[:, pl.ds(pl.multiple_of(step * BLK, BLK), BLK)] - update

    @pl.when(half == 1)
    def _():
        out_ref[...] = field_vmem[:, pl.ds(pl.multiple_of((step - 4) * BLK, BLK), BLK)] - update


def final(field0, field1, wide, *updates):
    return pl.pallas_call(
        final_kernel,
        grid=(ROWS // BLK,),
        out_shape=shape(COLS, ROWS),
        in_specs=[
            VMEM, HBM, HBM,
        ] + [VMEM] * 6,
        out_specs=pl.BlockSpec((COLS, BLK), lambda j: (0, j)),
        scratch_shapes=[
            pltpu.VMEM((COLS, 1024), BF16), pltpu.VMEM((COLS, UP), F32), pltpu.VMEM((512, ROWS), BF16),
            pltpu.VMEM((COLS, LEAF), F32), pltpu.SemaphoreType.DMA((12,)),
        ],
        compiler_params=params(20),
        cost_estimate=cost(2 * COLS * 1024 * ROWS, 12e6),
        name="final",
    )(field0, stay(field1), stay(wide), *updates)


def swap(array, mask, axis):
    return lax.ppermute(array, axis, [(i, i ^ mask) for i in range(lax.axis_size(axis))])


def local(samples, order_perm, leaf_factor, bases, coupling, ranks):
    wide, mine, theirs, own1, gram0, cross0, samples = grams(bases, samples)
    order = order_perm.reshape(1, ROWS)
    got = swap(theirs, 1, "core")
    sib1 = swap(own1, 1, "core")
    permuted0, factor = permute_first(samples, order, leaf_factor)
    permuted1 = permute_second(samples, order)
    field0 = leaf_product(permuted0, factor, 0)
    field1 = leaf_product(permuted1, factor, 1)
    q = project(field0, field1, wide)
    from0, weight1, onward1 = solve_early(ranks, coupling, gram0, own1, sib1)
    u0, u1, x, joint = early(ranks, coupling, q, from0, cross0, weight1, onward1)

    chip = (mine + got)[3:]
    got = swap(chip, 1, "z")
    low_lane = lax.broadcasted_iota(jnp.int32, (32, 128), 1) < R
    pack = [chip[0], got[1], got[2]]
    total = chip[3:] + got[3:]
    got = swap(total, 2, "z")
    pack += [jnp.where(low_lane, total[0], got[0]), got[1]]
    total = total[2:] + got[2:]
    got = swap(total, 7, "z")
    pack += [total[0], got[1]]
    total = total[2:] + got[2:]
    got = swap(total, 1, "x")
    pack += [jnp.where(low_lane, total[0], got[0]), total[1] + got[1]]
    near = jnp.stack(pack)
    far = swap(near, 1, "core")
    u1 = swap(u1, 1, "core")
    keep, send = late(ranks, joint, near, far, x)
    got = swap(send, 1, "core")
    two = level_two(keep, got)
    two = swap(two, 1, "z")
    dealt = deal(keep, got)
    got = lax.all_to_all(dealt, ("x", "z"), 0, 0, tiled=True)
    far_two = swap(two, 1, "core")
    total = collect(got)
    back = lax.all_to_all(total, ("x", "z"), 0, 0, tiled=True)
    far_back = swap(back, 1, "core")
    return final(field0, field1, wide, u0, u1, two, far_two, back, far_back)


def solution(mesh):
    fine = jax.sharding.Mesh(mesh.devices.reshape(4, 8, 2, 4), ("x", "z", "core", "cols"))
    leaf = ("x", "z", "core")
    in_specs = (
        P("cols", leaf),
        P(leaf),
        P(leaf, None, None),
        P(None, None, leaf),
        P(None, leaf, None, None),
        P(),
    )
    out_specs = P("cols", leaf)
    return jax.shard_map(local, mesh=fine, in_specs=in_specs, out_specs=out_specs, check_vma=False)
```

```python
import functools
import math

import jax
import jax.numpy as jnp
from jax import lax
from jax.experimental import pallas as pl
from jax.experimental.pallas import tpu as pltpu
from jax.sharding import PartitionSpec as P


F32, BF16 = jnp.float32, jnp.bfloat16
HIGH = lax.Precision.HIGHEST
NT = (((1,), (1,)), ((), ()))
NN = (((1,), (0,)), ((), ()))
TN = (((0,), (0,)), ((), ()))

LEAF, R, ROWS, COLS, LEVELS = 1024, 64, 2048, 512, 7
UP = (LEVELS - 1) * R
BLK = 256
WIDE = 512
MIB = 1024 * 1024
VMEM = pl.BlockSpec(memory_space=pltpu.VMEM)
SMEM = pl.BlockSpec(memory_space=pltpu.SMEM)
HBM = pl.BlockSpec(memory_space=pltpu.HBM)


def params(mib, **more):
    return pltpu.CompilerParams(vmem_limit_bytes=mib * MIB, **more)


def cost(flops, moved):
    return pl.CostEstimate(flops=int(flops), bytes_accessed=int(moved), transcendentals=0)


def shape(*dims, dtype=F32):
    return jax.ShapeDtypeStruct(dims, dtype)


def stay(array):
    return pltpu.with_memory_space_constraint(array, pltpu.HBM)


def split(value):
    high = value.astype(BF16)
    return high, (value - high.astype(F32)).astype(BF16)


def dot(left, right, dims):
    return lax.dot_general(left, right, dims, preferred_element_type=F32)


def dot_high(left, right, dims):
    return lax.dot_general(left, right, dims, precision=HIGH, preferred_element_type=F32)


def twice(value, axis):
    return jnp.concatenate([value, value], axis=axis)


def gram_kernel(bases_ref, samples_ref, wide_ref, mine_ref, theirs_ref, first_ref, gram0_ref, cross0_ref, kept_ref,
                held_ref, tiles_ref, sems):
    load = pltpu.make_async_copy(bases_ref, held_ref, sems.at[0])
    load.start()
    keep = pltpu.make_async_copy(samples_ref, kept_ref, sems.at[1])
    keep.start()
    load.wait()
    nothing = jnp.zeros((R, LEAF), BF16)
    wide_ref[0:UP] = held_ref[1:].reshape(UP, ROWS)
    wide_ref[UP:UP + R, 0:LEAF] = held_ref[0, :, 0:LEAF]
    wide_ref[UP:UP + R, LEAF:] = nothing
    wide_ref[UP + R:, 0:LEAF] = nothing
    wide_ref[UP + R:, LEAF:] = held_ref[0, :, LEAF:]
    wide = wide_ref[...]
    gram = dot(wide, wide, NT)
    first_ref[...] = gram[:R, :UP]
    tile = 0
    for level in range(6):
        for lane in range(level // 2, 3):
            for half in range(2):
                top = level * R + 32 * half
                tiles_ref[half, tile] = gram[top:top + 32, lane * 128:lane * 128 + 128]
            tile += 1
    core = lax.axis_index("core")
    mine_ref[...] = tiles_ref[core]
    theirs_ref[...] = tiles_ref[1 - core]
    gram0_ref[...] = gram[UP:, UP:]
    cross0_ref[...] = gram[UP:, :UP]
    keep.wait()


def grams(bases, samples):
    return pl.pallas_call(
        gram_kernel,
        out_shape=(
            shape(512, ROWS, dtype=BF16), shape(12, 32, 128), shape(12, 32, 128), shape(R, UP), shape(128, 128),
            shape(128, UP),
            pltpu.VMEM((COLS, ROWS), BF16),
        ),
        in_specs=[HBM] * 2,
        out_specs=(VMEM,) * 7,
        scratch_shapes=[pltpu.VMEM((LEVELS, R, ROWS), BF16), pltpu.VMEM((2, 12, 32, 128), F32), pltpu.SemaphoreType.DMA((2,))],
        compiler_params=params(14),
        cost_estimate=cost(2e9, 4e6),
        name="gram",
    )(stay(bases), stay(samples))


def permute_block(samples_ref, order_ref, out_ref, begin):
    def block(j, carry):
        columns = pl.ds(pl.multiple_of(j * BLK, BLK), BLK)
        rows = lax.broadcasted_iota(jnp.int32, (ROWS, BLK), 0)
        source = pl.ds(pl.multiple_of(begin + j * BLK, BLK), BLK)
        local = jnp.bitwise_and(order_ref[:, source], ROWS - 1)
        chosen = (rows == local).astype(F32).astype(BF16)
        out_ref[:, columns] = dot(samples_ref[...], chosen, NN).astype(BF16)
        return carry

    lax.fori_loop(0, LEAF // BLK, block, 0)


def permute_first_kernel(samples_ref, order_ref, factor_ref, out_ref, kept_ref, sem):
    keep = pltpu.make_async_copy(factor_ref, kept_ref, sem)
    keep.start()
    permute_block(samples_ref, order_ref, out_ref, 0)
    keep.wait()


def permute_second_kernel(samples_ref, order_ref, out_ref):
    permute_block(samples_ref, order_ref, out_ref, LEAF)


def permute_first(samples, order, factor):
    return pl.pallas_call(
        permute_first_kernel,
        out_shape=(shape(COLS, LEAF, dtype=BF16), pltpu.VMEM((2, LEAF, LEAF), BF16)),
        in_specs=[VMEM, VMEM, HBM],
        out_specs=(VMEM,) * 2,
        scratch_shapes=[pltpu.SemaphoreType.DMA],
        compiler_params=params(14),
        cost_estimate=cost(COLS * ROWS * ROWS, 4e6),
        name="permute_first",
    )(samples, order, stay(factor))


def permute_second(samples, order):
    return pl.pallas_call(
        permute_second_kernel,
        out_shape=shape(COLS, LEAF, dtype=BF16),
        in_specs=[VMEM, VMEM],
        out_specs=VMEM,
        compiler_params=params(10),
        cost_estimate=cost(COLS * ROWS * ROWS, 4e6),
        name="permute_second",
    )(samples, order)


def leaf_kernel(permuted_ref, factor_ref, field_ref, *, half):
    def block(j, carry):
        columns = pl.ds(pl.multiple_of(j * 512, 512), 512)
        field_ref[:, columns] = dot(permuted_ref[...], factor_ref[half, :, columns], NN)
        return carry

    lax.fori_loop(0, 2, block, 0)


def leaf_product(permuted, factor, half):
    return pl.pallas_call(
        functools.partial(leaf_kernel, half=half),
        out_shape=shape(COLS, LEAF),
        in_specs=[VMEM] * 2,
        out_specs=VMEM,
        compiler_params=params(12),
        cost_estimate=cost(2 * COLS * LEAF * LEAF, 5e6),
    )(permuted, factor)


def project_kernel(first_ref, second_ref, wide_ref, q_ref):
    def rows_of(i, carry):
        rows = pl.ds(pl.multiple_of(i * 256, 256), 256)
        total = None
        for half, source in enumerate((first_ref, second_ref)):
            for part in split(source[rows, :]):
                term = dot(part, wide_ref[:, half * LEAF:(half + 1) * LEAF], NT)
                total = term if total is None else total + term
        q_ref[rows, :] = total
        return carry

    lax.fori_loop(0, COLS // 256, rows_of, 0)


def project(first, second, wide):
    return pl.pallas_call(
        project_kernel,
        out_shape=shape(COLS, 512),
        in_specs=[VMEM] * 3,
        out_specs=VMEM,
        compiler_params=params(14),
        cost_estimate=cost(4 * COLS * 512 * ROWS, 7e6),
        name="project",
    )(first, second, wide)


def coupling_forms(link):
    flipped = link.T
    plain = twice(flipped, 0).T
    return plain, twice(link, 0).T


def lanes(rows=R):
    return lax.broadcasted_iota(jnp.int32, (rows, 128), 1)


def jointly(link_dup, rank_own, scale):
    return jnp.where(jnp.bitwise_and(lanes(), R - 1) < rank_own, link_dup * scale, 0.0)


def system(joint, gram_tile, upper_half):
    lane = lanes()
    placed = jnp.where((lane >= R) == upper_half, joint, 0.0)
    inner = dot_high(gram_tile, twice(placed, 0), NT)
    outer = dot_high(joint[:, :R], inner, NN)
    row = lax.broadcasted_iota(jnp.int32, (R, 128), 0)
    outer = outer + jnp.where(row == lane, 1.0, 0.0)
    return jnp.where(lane < R, outer, joint)


def eliminate(work_ref, count):
    row = lax.broadcasted_iota(jnp.int32, (count, R, 128), 1)
    tile_row = lax.broadcasted_iota(jnp.int32, (count, 8, 128), 1)
    value = work_ref[...]
    for top in range(0, R, 8):
        here = (row >= top) & (row < top + 8)
        tile = value[:, top:top + 8, :]
        heads = [jnp.broadcast_to(tile[:, :, j:j + 1], (count, 8, 128)) for j in range(top, top + 8)]
        columns = [jnp.broadcast_to(value[:, :, j:j + 1], (count, R, 128)) for j in range(top, top + 8)]
        for j in range(8):
            inverse = 1.0 / heads[j][:, j:j + 1, :]
            pivot = tile[:, j:j + 1, :] * inverse
            tile = jnp.where(tile_row == j, pivot, tile - heads[j] * pivot)
            for i in range(j + 1, 8):
                element = heads[i][:, j:j + 1, :] * inverse
                heads[i] = jnp.where(tile_row == j, element, heads[i] - heads[j] * element)
        for j in range(8):
            value = value - columns[j] * tile[:, j:j + 1, :]
        value = jnp.where(here, jnp.concatenate([tile] * 8, axis=1), value)
    work_ref[...] = pltpu.roll(value, R, 2)


def solved(work_ref, item, rank_sibling, scale):
    row = lax.broadcasted_iota(jnp.int32, (R, 128), 0)
    keep = (row < rank_sibling) & (lanes() < R)
    return jnp.where(keep, work_ref[item] * scale, 0.0)


def pair(value):
    high, low = split(value)
    return jnp.concatenate([high, low], axis=1)


def apply_nt(value_pair, weight):
    high, low = split(weight)
    return dot(value_pair, twice(high, 1), NT) + dot(value_pair, twice(low, 1), NT)


def apply_nn(value_pair, weight):
    high, low = split(weight)
    return dot(value_pair, twice(high, 0), NN) + dot(value_pair, twice(low, 0), NN)


def packed(value_pair, weight):
    nothing = jnp.zeros_like(weight)
    left = jnp.concatenate([value_pair[0:128], value_pair[256:384]], axis=0)
    right = jnp.concatenate([value_pair[128:256], value_pair[384:512]], axis=0)
    return apply_nt(left, jnp.concatenate([weight, nothing], 0)) + apply_nt(right, jnp.concatenate([nothing, weight], 0))


def leaf_index():
    return (lax.axis_index("x") * 8 + lax.axis_index("z")) * 2 + lax.axis_index("core")


def scale_of(level):
    return 1.0 / math.sqrt(LEAF * 2**level)


def solve_early_kernel(ranks_ref, link_ref, gram0_ref, own1_ref, sib1_ref, from0_ref, weight_ref, onward_ref, work_ref):
    leaf = leaf_index()
    second = lax.axis_index("core")
    plain0, flipped0 = coupling_forms(link_ref[0, 0])
    plain1, flipped1 = coupling_forms(link_ref[1, 0])
    rank_f, rank_s = ranks_ref[0, 2 * leaf], ranks_ref[0, 2 * leaf + 1]
    rank_1, rank_1s = ranks_ref[1, 2 * leaf], ranks_ref[1, 2 * jnp.bitwise_xor(leaf, 1)]
    scale0, scale1 = scale_of(0), scale_of(1)
    work_ref[0] = system(jointly(flipped0, rank_f, scale0), gram0_ref[0:R], False)
    work_ref[1] = system(jointly(plain0, rank_s, scale0), gram0_ref[R:], True)
    joint1 = jointly(jnp.where(second == 1, plain1, flipped1), rank_1, scale1)
    work_ref[2] = system(joint1, own1_ref[:, :128], False)
    eliminate(work_ref, 3)
    from0_ref[R:] = solved(work_ref, 0, rank_s, scale0)
    from0_ref[0:R] = pltpu.roll(solved(work_ref, 1, rank_f, scale0), R, 1)
    weight = solved(work_ref, 2, rank_1s, scale1)
    weight_ref[...] = weight
    onward_ref[...] = dot_high(weight, sib1_ref[...], TN)


def solve_early(ranks, coupling, gram0, own1, sib1):
    return pl.pallas_call(
        solve_early_kernel,
        out_shape=(shape(128, 128), shape(R, 128), shape(128, UP)),
        in_specs=[SMEM] + [VMEM] * 4,
        out_specs=(VMEM,) * 3,
        scratch_shapes=[pltpu.VMEM((3, R, 128), F32)],
        compiler_params=params(8),
        cost_estimate=cost(3e9, 4e6),
        name="solve_early",
    )(ranks, coupling, gram0, own1, sib1)


def early_kernel(ranks_ref, link_ref, q_ref, from0_ref, cross0_ref, weight_ref, onward_ref,
                 u0_ref, u1_ref, x_ref, joint_ref):
    leaf = leaf_index()
    for level in range(2, 7):
        child = jnp.right_shift(leaf, level - 1)
        plain, flipped = coupling_forms(link_ref[level, 0])
        rank = ranks_ref[level, jnp.left_shift(child, level)]
        which = jnp.where(jnp.bitwise_and(child, 1) == 1, plain, flipped)
        joint_ref[level - 2] = jointly(which, rank, scale_of(level))
    u0 = apply_nt(pair(q_ref[:, UP:]), from0_ref[...])
    u0_ref[...] = u0
    zero = pair(u0)
    cross0 = cross0_ref[...]
    head = pair(q_ref[:, :128] - apply_nn(zero, cross0[:, :128]))
    both = packed(head, weight_ref[...])
    u1_ref[0] = both[:128]
    u1_ref[1] = both[128:]
    onward = onward_ref[...]
    for group in range(3):
        at = slice(group * 128, group * 128 + 128)
        x_ref[:, at] = q_ref[:, at] - apply_nn(zero, cross0[:, at]) - apply_nn(head, onward[:, at])


def early(ranks, coupling, q, from0, cross0, weight, onward):
    return pl.pallas_call(
        early_kernel,
        out_shape=(shape(COLS, 128), shape(2, 128, 128), shape(COLS, UP), shape(5, R, 128)),
        in_specs=[SMEM] + [VMEM] * 6,
        out_specs=(VMEM,) * 4,
        compiler_params=params(12),
        cost_estimate=cost(3e9, 4e6),
        name="early",
    )(ranks, coupling, q, from0, cross0, weight, onward)


OWN_TILE = {2: 0, 3: 3, 4: 5, 5: 7, 6: 8}
ONWARD = {2: ((1, 1), (2, 2)), 3: ((3, 1), (4, 2)), 4: ((6, 2),), 5: ((7, 2),), 6: ()}


def late_kernel(ranks_ref, joint_ref, near_ref, far_ref, x_ref, keep_ref, send_ref, pk_ref, work_ref):
    leaf, core = leaf_index(), lax.axis_index("core")
    for other, source in ((0, near_ref), (1, far_ref)):
        rows = pl.ds(pl.multiple_of(jnp.bitwise_xor(core, other) * 32, 32), 32)
        for tile in range(9):
            pk_ref[tile, rows, :] = source[tile]
    systems = []
    for level in range(2, 7):
        systems.append(system(joint_ref[level - 2], pk_ref[OWN_TILE[level]], level % 2 == 0))
    for item in range(5):
        work_ref[item] = systems[item]
    eliminate(work_ref, 5)
    weights, onwards = {}, {}
    for level in range(2, 7):
        child = jnp.right_shift(leaf, level - 1)
        rank = ranks_ref[level, jnp.left_shift(jnp.bitwise_xor(child, 1), level)]
        weight = solved(work_ref, level - 2, rank, scale_of(level))
        if level % 2 == 0:
            weight = pltpu.roll(weight, R, 1)
        weights[level] = weight
        onwards[level] = [(dot_high(weight, pk_ref[tile], TN), target) for tile, target in ONWARD[level]]
    groups = [x_ref[:, g * 128:g * 128 + 128] for g in range(3)]
    for level in range(2, 7):
        value = pair(groups[(level - 1) // 2])
        for onward, target in onwards[level]:
            groups[target] = groups[target] - apply_nn(value, onward)
        both = packed(value, weights[level])
        keep_ref[level - 2] = jnp.where(core == 0, both[:128], both[128:])
        send_ref[level - 2] = jnp.where(core == 0, both[128:], both[:128])


def late(ranks, joint, near, far, x):
    return pl.pallas_call(
        late_kernel,
        out_shape=(shape(5, 128, 128), shape(5, 128, 128)),
        in_specs=[SMEM] + [VMEM] * 4,
        out_specs=(VMEM,) * 2,
        scratch_shapes=[pltpu.VMEM((9, R, 128), F32), pltpu.VMEM((5, R, 128), F32)],
        compiler_params=params(16),
        cost_estimate=cost(4e9, 4e6),
        name="late",
    )(ranks, joint, near, far, x)


def turned(value):
    return pltpu.roll(value, 4, 0)


def two_kernel(keep_ref, recv_ref, two_ref):
    two_ref[...] = keep_ref[0] + recv_ref[0]


def level_two(keep, recv):
    return pl.pallas_call(
        two_kernel,
        out_shape=shape(128, 128),
        in_specs=[VMEM] * 2,
        out_specs=VMEM,
        compiler_params=params(4),
        cost_estimate=cost(1e6, 1e5),
        name="two",
    )(keep, recv)


def deal_kernel(keep_ref, recv_ref, out_ref):
    top = lax.broadcasted_iota(jnp.int32, (8, 128), 0) < 4
    for t in range(16):
        rows = slice(8 * t, 8 * t + 8)
        for group in range(2):
            first = keep_ref[2 * group + 1, rows] + recv_ref[2 * group + 1, rows]
            second = keep_ref[2 * group + 2, rows] + recv_ref[2 * group + 2, rows]
            to = slice(8 * group, 8 * group + 8)
            out_ref[2 * t, to] = jnp.where(top, first, turned(second))
            out_ref[2 * t + 1, to] = jnp.where(top, turned(first), second)


def deal(keep, recv):
    return pl.pallas_call(
        deal_kernel,
        out_shape=shape(32, 16, 128),
        in_specs=[VMEM] * 2,
        out_specs=VMEM,
        compiler_params=params(4),
        cost_estimate=cost(1e8, 1e6),
        name="deal",
    )(keep, recv)


def collect_kernel(got_ref, out_ref):
    top = lax.broadcasted_iota(jnp.int32, (8, 128), 0) < 4
    pieces = [got_ref[q] for q in range(32)]
    sums = []
    for _ in range(4):
        pieces = [pieces[2 * c] + pieces[2 * c + 1] for c in range(len(pieces) // 2)]
        sums.append(pieces)
    for e in range(32):
        parts = [sums[k][(e >> (k + 1)) ^ 1] for k in range(4)]
        out_ref[e, 0:8] = jnp.where(top, parts[0][0:8], parts[1][0:8])
        out_ref[e, 8:16] = jnp.where(top, parts[2][8:16], parts[3][8:16])


def collect(got):
    return pl.pallas_call(
        collect_kernel,
        out_shape=shape(32, 16, 128),
        in_specs=[VMEM],
        out_specs=VMEM,
        compiler_params=params(4),
        cost_estimate=cost(1e8, 1e6),
        name="collect",
    )(got)


def final_kernel(field0_ref, field1_ref, wide_ref, u0_ref, u1_ref, near2_ref, far2_ref, near_ref, far_ref,
                 out_ref, left_ref, all_ref, wide_vmem, field_vmem, sems):
    step = pl.program_id(0)
    half = step // (LEAF // WIDE)
    loads = [
        pltpu.make_async_copy(
            wide_ref.at[:, j * WIDE:j * WIDE + WIDE], wide_vmem.at[:, j * WIDE:j * WIDE + WIDE], sems.at[j]
        )
        for j in range(4)
    ]
    loads += [
        pltpu.make_async_copy(
            field1_ref.at[:, j * WIDE:j * WIDE + WIDE], field_vmem.at[:, j * WIDE:j * WIDE + WIDE], sems.at[4 + j]
        )
        for j in range(2)
    ]

    @pl.when(step == 0)
    def _():
        for load in loads:
            load.start()
        core = lax.axis_index("core")
        top = lax.broadcasted_iota(jnp.int32, (8, 128), 0) < 4
        lane = lanes(8)

        def unpack(first, second, begin, group):
            columns = slice(group * 128, group * 128 + 128)
            upper = pl.ds(pl.multiple_of(begin, 8), 8)
            lower = pl.ds(pl.multiple_of(begin + 128, 8), 8)
            all_ref[upper, columns] = jnp.where(lane < R, first, pltpu.roll(second, R, 1))
            all_ref[lower, columns] = jnp.where(lane < R, pltpu.roll(first, R, 1), second)

        for two, rest, start in ((near2_ref, near_ref, core), (far2_ref, far_ref, 1 - core)):
            for t in range(16):
                rows = slice(8 * t, 8 * t + 8)
                begin = start * 256 + 8 * t
                unpack(u1_ref[start, rows], two[rows], begin, 0)
                for group in range(2):
                    one = rest[2 * t, 8 * group:8 * group + 8]
                    other = rest[2 * t + 1, 8 * group:8 * group + 8]
                    unpack(
                        jnp.where(top, one, turned(other)), jnp.where(top, turned(one), other), begin, group + 1
                    )
        high, low = split(all_ref[...])
        left_ref[:, 0:UP] = high
        left_ref[:, 512:512 + UP] = low
        high, low = split(u0_ref[...])
        left_ref[:, UP:512] = high
        left_ref[:, 512 + UP:] = low

    for j in range(4):
        @pl.when(step == j)
        def _():
            loads[j].wait()
            if j >= 2:
                loads[j + 2].wait()

    right = wide_vmem[:, pl.ds(pl.multiple_of(step * WIDE, WIDE), WIDE)]
    update = dot(left_ref[:, :512], right, NN) + dot(left_ref[:, 512:], right, NN)

    @pl.when(half == 0)
    def _():
        out_ref[...] = field0_ref[:, pl.ds(pl.multiple_of(step * WIDE, WIDE), WIDE)] - update

    @pl.when(half == 1)
    def _():
        out_ref[...] = field_vmem[:, pl.ds(pl.multiple_of((step - 2) * WIDE, WIDE), WIDE)] - update


def final(field0, field1, wide, *updates):
    return pl.pallas_call(
        final_kernel,
        grid=(ROWS // WIDE,),
        out_shape=shape(COLS, ROWS),
        in_specs=[
            VMEM, HBM, HBM,
        ] + [VMEM] * 6,
        out_specs=pl.BlockSpec((COLS, WIDE), lambda j: (0, j)),
        scratch_shapes=[
            pltpu.VMEM((COLS, 1024), BF16), pltpu.VMEM((COLS, UP), F32), pltpu.VMEM((512, ROWS), BF16),
            pltpu.VMEM((COLS, LEAF), F32), pltpu.SemaphoreType.DMA((6,)),
        ],
        compiler_params=params(20),
        cost_estimate=cost(2 * COLS * 1024 * ROWS, 12e6),
        name="final",
    )(field0, stay(field1), stay(wide), *updates)


def swap(array, mask, axis):
    return lax.ppermute(array, axis, [(i, i ^ mask) for i in range(lax.axis_size(axis))])


def local(samples, order_perm, leaf_factor, bases, coupling, ranks):
    wide, mine, theirs, own1, gram0, cross0, samples = grams(bases, samples)
    order = order_perm.reshape(1, ROWS)
    got = swap(theirs, 1, "core")
    sib1 = swap(own1, 1, "core")
    permuted0, factor = permute_first(samples, order, leaf_factor)
    permuted1 = permute_second(samples, order)
    field0 = leaf_product(permuted0, factor, 0)
    field1 = leaf_product(permuted1, factor, 1)
    q = project(field0, field1, wide)
    from0, weight1, onward1 = solve_early(ranks, coupling, gram0, own1, sib1)
    u0, u1, x, joint = early(ranks, coupling, q, from0, cross0, weight1, onward1)

    chip = (mine + got)[3:]
    got = swap(chip, 1, "z")
    low_lane = lax.broadcasted_iota(jnp.int32, (32, 128), 1) < R
    pack = [chip[0], got[1], got[2]]
    total = chip[3:] + got[3:]
    got = swap(total, 2, "z")
    pack += [jnp.where(low_lane, total[0], got[0]), got[1]]
    total = total[2:] + got[2:]
    got = swap(total, 7, "z")
    pack += [total[0], got[1]]
    total = total[2:] + got[2:]
    got = swap(total, 1, "x")
    pack += [jnp.where(low_lane, total[0], got[0]), total[1] + got[1]]
    near = jnp.stack(pack)
    far = swap(near, 1, "core")
    u1 = swap(u1, 1, "core")
    keep, send = late(ranks, joint, near, far, x)
    got = swap(send, 1, "core")
    two = level_two(keep, got)
    two = swap(two, 1, "z")
    dealt = deal(keep, got)
    got = lax.all_to_all(dealt, ("x", "z"), 0, 0, tiled=True)
    far_two = swap(two, 1, "core")
    total = collect(got)
    back = lax.all_to_all(total, ("x", "z"), 0, 0, tiled=True)
    far_back = swap(back, 1, "core")
    return final(field0, field1, wide, u0, u1, two, far_two, back, far_back)


def solution(mesh):
    fine = jax.sharding.Mesh(mesh.devices.reshape(4, 8, 2, 4), ("x", "z", "core", "cols"))
    leaf = ("x", "z", "core")
    in_specs = (
        P("cols", leaf),
        P(leaf),
        P(leaf, None, None),
        P(None, None, leaf),
        P(None, leaf, None, None),
        P(),
    )
    out_specs = P("cols", leaf)
    return jax.shard_map(local, mesh=fine, in_specs=in_specs, out_specs=out_specs, check_vma=False)
```
